128 devices in a mesh: dp: 1, tp: 2 (over core), sp: 64 (over z, y, x).
Axes of the slice: x: 4, y: 4, z: 4, core: 2. Of those that a mesh axis runs over, the one named last changes fastest.
Arguments:
- tok_emb: bfloat16 [4, 32, 2048], P(None, 'dp')
- lengths: int32 [32], P('dp')
- key_cache: bfloat16 [2, 32, 8192, 2, 128], P(None, 'dp', 'sp', 'tp')
- val_cache: bfloat16 [2, 32, 8192, 2, 128], P(None, 'dp', 'sp', 'tp')
- gain_attn: bfloat16 [2, 2048], replicated
- gain_mlp: bfloat16 [2, 2048], replicated
- w_query: bfloat16 [2, 2048, 2048], P(None, None, 'tp')
- w_key: bfloat16 [2, 2048, 256], P(None, None, 'tp')
- w_value: bfloat16 [2, 2048, 256], P(None, None, 'tp')
- w_out: bfloat16 [2, 2048, 2048], P(None, 'tp')
- w_gate: bfloat16 [2, 2048, 11008], P(None, None, 'tp')
- w_up: bfloat16 [2, 2048, 11008], P(None, None, 'tp')
- w_down: bfloat16 [2, 11008, 2048], P(None, 'tp')
Outputs:
- output 1: bfloat16 [4, 32, 2048], P(None, 'dp')
- output 2: bfloat16 [2, 32, 8192, 2, 128], P(None, 'dp', 'sp', 'tp')
- output 3: bfloat16 [2, 32, 8192, 2, 128], P(None, 'dp', 'sp', 'tp')
All inputs are finite; a program needn't handle non-finite values.
Results may differ from the reference program's by a relative error of at most 0.0153106.
Values sent between devices are 32-bit elements.
A program may use at most 1 GiB of HBM per device.

```python
import math
import jax
import jax.numpy as jnp
from jax import lax

N_STEPS = 4
N_LAYERS = 2
SEQ_BATCH = 32
LOC_LEN = 128
SP_SIZE = 64
D_MODEL = 2048
N_HEADS = 16
KV_HEADS = 2
HEAD_DIM = 128
FF_DIM = 11008
CACHE_LEN = LOC_LEN * SP_SIZE
GROUP_SIZE = N_HEADS // KV_HEADS
EPS = 1e-5
ROPE_BASE = 500000.0


def draw_lengths(len_key, perm_key):
    drawn_len = jax.random.randint(len_key, (SEQ_BATCH,), CACHE_LEN // 2, CACHE_LEN - N_STEPS + 1)
    perm_ids = jax.random.permutation(perm_key, SEQ_BATCH)
    lengths = jnp.where(perm_ids == 0, CACHE_LEN - N_STEPS, jnp.where(perm_ids == 1, CACHE_LEN // 2, drawn_len))
    return lengths.astype(jnp.int32)


def draw_scales():
    score_var = max(math.log(CACHE_LEN / 32.0), 1.0)
    plant_gain = (math.log(CACHE_LEN) + 0.5 * score_var) / math.sqrt(HEAD_DIM)
    key_scale = math.sqrt(score_var / (1.0 + plant_gain * plant_gain))
    return plant_gain, key_scale


def setup_inputs(seed: int = 0, part: int = 0) -> dict:
    plant_gain, key_scale = draw_scales()
    part_keys = jax.random.split(jax.random.fold_in(jax.random.key(seed), part), 6)
    weight_keys = jax.random.split(jax.random.key(seed + 1), 9)
    common = jax.random.normal(part_keys[0], (SEQ_BATCH, D_MODEL), jnp.float32)
    step_noise = jax.random.normal(part_keys[1], (N_STEPS, SEQ_BATCH, D_MODEL), jnp.float32)
    tok_emb = ((common[None] + 0.4 * step_noise) / math.sqrt(1.16)).astype(jnp.bfloat16)
    lengths = draw_lengths(part_keys[2], part_keys[3])
    cache_shape = (N_LAYERS, SEQ_BATCH, CACHE_LEN, KV_HEADS, HEAD_DIM)
    key_cache = (key_scale * jax.random.normal(part_keys[4], cache_shape, jnp.float32)).astype(jnp.bfloat16)
    val_cache = jax.random.normal(part_keys[5], cache_shape, jnp.float32).astype(jnp.bfloat16)
    gain_attn = (1.0 + 0.3 * jax.random.normal(weight_keys[0], (N_LAYERS, D_MODEL), jnp.float32)).astype(jnp.bfloat16)
    gain_mlp = (1.0 + 0.3 * jax.random.normal(weight_keys[1], (N_LAYERS, D_MODEL), jnp.float32)).astype(jnp.bfloat16)
    in_scale = D_MODEL ** -0.5
    key_proj = jax.random.normal(weight_keys[2], (N_LAYERS, D_MODEL, KV_HEADS, HEAD_DIM), jnp.float32) * in_scale
    query_proj = plant_gain * jnp.repeat(key_proj, GROUP_SIZE, axis=2) + jax.random.normal(weight_keys[3], (N_LAYERS, D_MODEL, N_HEADS, HEAD_DIM), jnp.float32) * in_scale
    w_query = query_proj.reshape(N_LAYERS, D_MODEL, N_HEADS * HEAD_DIM).astype(jnp.bfloat16)
    w_key = key_proj.reshape(N_LAYERS, D_MODEL, KV_HEADS * HEAD_DIM).astype(jnp.bfloat16)
    w_value = (jax.random.normal(weight_keys[4], (N_LAYERS, D_MODEL, KV_HEADS * HEAD_DIM), jnp.float32) * in_scale).astype(jnp.bfloat16)
    w_out = (jax.random.normal(weight_keys[5], (N_LAYERS, N_HEADS * HEAD_DIM, D_MODEL), jnp.float32) * (N_HEADS * HEAD_DIM) ** -0.5).astype(jnp.bfloat16)
    w_gate = (jax.random.normal(weight_keys[6], (N_LAYERS, D_MODEL, FF_DIM), jnp.float32) * in_scale).astype(jnp.bfloat16)
    w_up = (jax.random.normal(weight_keys[7], (N_LAYERS, D_MODEL, FF_DIM), jnp.float32) * in_scale).astype(jnp.bfloat16)
    w_down = (jax.random.normal(weight_keys[8], (N_LAYERS, FF_DIM, D_MODEL), jnp.float32) * FF_DIM ** -0.5).astype(jnp.bfloat16)
    return {'tok_emb': tok_emb, 'lengths': lengths, 'key_cache': key_cache, 'val_cache': val_cache, 'gain_attn': gain_attn, 'gain_mlp': gain_mlp, 'w_query': w_query, 'w_key': w_key, 'w_value': w_value, 'w_out': w_out, 'w_gate': w_gate, 'w_up': w_up, 'w_down': w_down}


def rms_norm(hidden, gain_vec):
    x_float = hidden.astype(jnp.float32)
    inv_rms = lax.rsqrt(jnp.mean(x_float * x_float, axis=-1, keepdims=True) + EPS)
    return (x_float * inv_rms * gain_vec.astype(jnp.float32)).astype(jnp.bfloat16)


def rotary(in_vecs, positions):
    head_dim = in_vecs.shape[-1]
    half_dim = head_dim // 2
    inv_freq = 1.0 / (ROPE_BASE ** (jnp.arange(half_dim).astype(jnp.float32) * 2.0 / head_dim))
    angles = positions.astype(jnp.float32)[:, None] * inv_freq[None, :]
    cos_a = jnp.cos(angles)[:, None, :]
    sin_a = jnp.sin(angles)[:, None, :]
    front_half = in_vecs[..., :half_dim]
    back_half = in_vecs[..., half_dim:]
    return jnp.concatenate([front_half * cos_a - back_half * sin_a, back_half * cos_a + front_half * sin_a], axis=-1)


def reference(tok_emb, lengths, key_cache, val_cache, gain_attn, gain_mlp, w_query, w_key, w_value, w_out, w_gate, w_up, w_down):
    slot_ids = jnp.arange(CACHE_LEN)
    slot_pos = (slot_ids % LOC_LEN) * SP_SIZE + slot_ids // LOC_LEN
    row_ids = jnp.arange(SEQ_BATCH)

    def one_step(caches, step_in):
        step_idx, hidden = step_in
        cur_pos = lengths + step_idx
        write_slot = (cur_pos % SP_SIZE) * LOC_LEN + cur_pos // SP_SIZE
        valid_mask = (slot_pos[None, :] <= cur_pos[:, None])[:, None, None, :]

        def one_layer(hidden, layer_in):
            lay_k, lay_v, gain_a, gain_m, lay_wq, lay_wk, lay_wv, lay_wo, lay_wg, lay_wu, lay_wd = layer_in
            normed = rms_norm(hidden, gain_a)
            q_vec = jnp.dot(normed, lay_wq, preferred_element_type=jnp.float32).reshape(SEQ_BATCH, N_HEADS, HEAD_DIM)
            k_vec = jnp.dot(normed, lay_wk, preferred_element_type=jnp.float32).reshape(SEQ_BATCH, KV_HEADS, HEAD_DIM)
            v_vec = jnp.dot(normed, lay_wv, preferred_element_type=jnp.float32).reshape(SEQ_BATCH, KV_HEADS, HEAD_DIM).astype(jnp.bfloat16)
            q_rot = rotary(q_vec, cur_pos).astype(jnp.bfloat16).reshape(SEQ_BATCH, KV_HEADS, GROUP_SIZE, HEAD_DIM)
            k_rot = rotary(k_vec, cur_pos).astype(jnp.bfloat16)
            lay_k = lay_k.at[row_ids, write_slot].set(k_rot)
            lay_v = lay_v.at[row_ids, write_slot].set(v_vec)
            scores = jnp.einsum('bkgd,bjkd->bkgj', q_rot.astype(jnp.float32), lay_k.astype(jnp.float32)) * HEAD_DIM ** -0.5
            scores = jnp.where(valid_mask, scores, -1e30)
            prob_w = jnp.exp(scores - jnp.max(scores, axis=-1, keepdims=True))
            denom_sum = jnp.sum(prob_w, axis=-1, keepdims=True)
            numer_sum = jnp.einsum('bkgj,bjkd->bkgd', prob_w.astype(jnp.bfloat16).astype(jnp.float32), lay_v.astype(jnp.float32))
            attn_out = (numer_sum / denom_sum).astype(jnp.bfloat16).reshape(SEQ_BATCH, N_HEADS * HEAD_DIM)
            hidden = (hidden.astype(jnp.float32) + jnp.dot(attn_out, lay_wo, preferred_element_type=jnp.float32)).astype(jnp.bfloat16)
            normed = rms_norm(hidden, gain_m)
            gate_pre = jnp.dot(normed, lay_wg, preferred_element_type=jnp.float32)
            up_pre = jnp.dot(normed, lay_wu, preferred_element_type=jnp.float32)
            mlp_act = (jax.nn.silu(gate_pre) * up_pre).astype(jnp.bfloat16)
            hidden = (hidden.astype(jnp.float32) + jnp.dot(mlp_act, lay_wd, preferred_element_type=jnp.float32)).astype(jnp.bfloat16)
            return hidden, (lay_k, lay_v)

        hidden, new_caches = lax.scan(one_layer, hidden, (caches[0], caches[1], gain_attn, gain_mlp, w_query, w_key, w_value, w_out, w_gate, w_up, w_down))
        return new_caches, hidden

    final_caches, hidden_all = lax.scan(one_step, (key_cache, val_cache), (jnp.arange(N_STEPS), tok_emb))
    return (hidden_all, final_caches[0], final_caches[1])
```

```python
import jax
import jax.numpy as jnp
from jax import lax
from jax.sharding import PartitionSpec as P

EPS = 1e-5
ROPE_BASE = 500000.0


def rms_norm(hidden, gain_vec):
    x_float = hidden.astype(jnp.float32)
    inv_rms = lax.rsqrt(jnp.mean(x_float * x_float, axis=-1, keepdims=True) + EPS)
    return (x_float * inv_rms * gain_vec.astype(jnp.float32)).astype(jnp.bfloat16)


def rotary(in_vecs, positions):
    head_dim = in_vecs.shape[-1]
    half_dim = head_dim // 2
    inv_freq = 1.0 / (ROPE_BASE ** (jnp.arange(half_dim).astype(jnp.float32) * 2.0 / head_dim))
    angles = positions.astype(jnp.float32)[:, None] * inv_freq[None, :]
    cos_a = jnp.cos(angles)[:, None, :]
    sin_a = jnp.sin(angles)[:, None, :]
    front_half = in_vecs[..., :half_dim]
    back_half = in_vecs[..., half_dim:]
    return jnp.concatenate([front_half * cos_a - back_half * sin_a, back_half * cos_a + front_half * sin_a], axis=-1)


def project(normed, weight):
    return jnp.dot(normed, weight, preferred_element_type=jnp.float32)


def solution(mesh):
    sp_size = mesh.shape['sp']

    def local_fn(tok_emb, lengths, key_cache, val_cache, gain_attn, gain_mlp, w_query, w_key, w_value, w_out, w_gate, w_up, w_down):
        n_steps, n_batch, width = tok_emb.shape
        n_layers, _, loc_len, kv_loc, head_dim = key_cache.shape
        heads_loc = w_query.shape[2] // head_dim
        group_size = heads_loc // kv_loc
        n_tok = n_steps * n_batch
        my_sp = lax.axis_index('sp')
        slot_pos = jnp.arange(loc_len) * sp_size + my_sp
        cur_pos = lengths[:, None] + jnp.arange(n_steps)[None, :]
        tok_pos = cur_pos.reshape(n_tok)
        write_slot = jnp.where(cur_pos % sp_size == my_sp, cur_pos // sp_size, loc_len)
        valid_mask = (slot_pos[None, None, :] <= cur_pos[:, :, None])[:, None, :, None, :]
        row_ids = jnp.arange(n_batch)[:, None]
        new_keys = key_cache
        new_vals = val_cache
        hidden = jnp.swapaxes(tok_emb, 0, 1).reshape(n_tok, width)
        for layer_idx in range(n_layers):
            normed = rms_norm(hidden, gain_attn[layer_idx])
            q_vec = project(normed, w_query[layer_idx]).reshape(n_tok, heads_loc, head_dim)
            k_vec = project(normed, w_key[layer_idx]).reshape(n_tok, kv_loc, head_dim)
            v_vec = project(normed, w_value[layer_idx]).astype(jnp.bfloat16)
            q_rot = rotary(q_vec, tok_pos).astype(jnp.bfloat16).reshape(n_batch, n_steps, kv_loc, group_size, head_dim)
            k_rot = rotary(k_vec, tok_pos).astype(jnp.bfloat16).reshape(n_batch, n_steps, kv_loc, head_dim)
            new_keys = new_keys.at[layer_idx, row_ids, write_slot].set(k_rot, mode='drop')
            new_vals = new_vals.at[layer_idx, row_ids, write_slot].set(v_vec.reshape(n_batch, n_steps, kv_loc, head_dim), mode='drop')
            scores = jnp.einsum('bskgd,bjkd->bksgj', q_rot, new_keys[layer_idx], preferred_element_type=jnp.float32) * head_dim ** -0.5
            scores = jnp.where(valid_mask, scores, -1e30)
            loc_max = jnp.max(scores, axis=-1, keepdims=True)
            prob_w = jnp.exp(scores - loc_max)
            loc_sum = jnp.sum(prob_w, axis=-1, keepdims=True)
            loc_out = jnp.einsum('bksgj,bjkd->bksgd', prob_w.astype(jnp.bfloat16), new_vals[layer_idx], preferred_element_type=jnp.float32)
            glob_max = lax.pmax(loc_max, 'sp')
            rescale = jnp.exp(loc_max - glob_max)
            merged = lax.psum(jnp.concatenate([loc_out, loc_sum], axis=-1) * rescale, 'sp')
            attn_out = (merged[..., :head_dim] / merged[..., head_dim:]).astype(jnp.bfloat16)
            attn_out = jnp.swapaxes(attn_out, 1, 2).reshape(n_tok, heads_loc * head_dim)
            proj_sum = lax.psum(project(attn_out, w_out[layer_idx]), 'tp')
            hidden = (hidden.astype(jnp.float32) + proj_sum).astype(jnp.bfloat16)
            normed = rms_norm(hidden, gain_mlp[layer_idx])
            mlp_act = (jax.nn.silu(project(normed, w_gate[layer_idx])) * project(normed, w_up[layer_idx])).astype(jnp.bfloat16)
            down_sum = lax.psum(project(mlp_act, w_down[layer_idx]), 'tp')
            hidden = (hidden.astype(jnp.float32) + down_sum).astype(jnp.bfloat16)
        hidden = jnp.swapaxes(hidden.reshape(n_batch, n_steps, width), 0, 1)
        return hidden, new_keys, new_vals

    cache_spec = P(None, 'dp', 'sp', 'tp', None)
    col_spec = P(None, None, 'tp')
    row_spec = P(None, 'tp', None)
    emb_spec = P(None, 'dp', None)
    return jax.shard_map(local_fn, mesh=mesh, in_specs=(emb_spec, P('dp'), cache_spec, cache_spec, P(), P(), col_spec, col_spec, col_spec, row_spec, col_spec, col_spec, row_spec), out_specs=(emb_spec, cache_spec, cache_spec), check_vma=False)
```

```python
import functools

import jax
import jax.numpy as jnp
from jax import lax
from jax.experimental import pallas as pl
from jax.experimental.pallas import tpu as pltpu
from jax.sharding import PartitionSpec as P

EPS = 1e-5
ROPE_BASE = 500000.0
CHUNK = 512
SLOTS = 6
UNROLL = 8
F32 = jnp.float32
BF16 = jnp.bfloat16
MESH = pl.DeviceIdType.MESH


def dot(a, b):
    return jnp.dot(a, b, preferred_element_type=F32)


def norm(u, gain):
    inv = lax.rsqrt(jnp.mean(u * u, axis=-1, keepdims=True) + EPS)
    return (u * inv * gain).astype(BF16)


def iota(shape, dim):
    return lax.broadcasted_iota(jnp.int32, shape, dim)


def kernel(sp, n_steps, n_batch, side,
           len_ref, freq_ref, ga_ref, gm_ref, x_hbm, kc_hbm, vc_hbm, wq_hbm, wk_hbm, wv_hbm, wo_hbm, wg_hbm, wu_hbm, wd_hbm,
           hid_hbm, ko_hbm, vo_hbm,
           x_v, xn_v, wqkv_v, wo_v, kc_v, vc_v, wg_v, wu_v, wd_v, q0_v, k0_v, v0_v,
           q_recv, kv_recv, o_send, o_recv, st_send, st_recv, x_send, x_recv, acc_v, q_send, kv_send, h_send,
           h_recv, h_other, out_v, tr_v, at_v,
           in_sem, cache_sem, out_sem, wqkv_sem, wo_sem, slot_sem,
           o_ssem, o_rsem, st_ssem, st_rsem, x_ssem, x_rsem, ag_ssem, ag_rsem):
    me = lax.axis_index('sp')
    core = lax.axis_index('tp')
    n_tok = n_steps * n_batch
    width = x_v.shape[1]
    d = 128
    ff = wg_hbm.shape[2]
    heads = wq_hbm.shape[2] // d
    qw = heads * d
    n_chunks = -(-ff // CHUNK)
    total = 2 * n_chunks
    last = sp - 1
    partner = {'tp': 1 - core}

    def local(src, dst, sem):
        return pltpu.make_async_copy(src, dst, sem)

    def remote(src, dst, ssem, rsem, dev):
        return pltpu.make_async_remote_copy(src_ref=src, dst_ref=dst, send_sem=ssem, recv_sem=rsem, device_id=dev, device_id_type=MESH)

    def qkv_copies(lay):
        return (local(wq_hbm.at[lay], wqkv_v.at[:, pl.ds(0, qw)], wqkv_sem.at[0]),
                local(wk_hbm.at[lay], wqkv_v.at[:, pl.ds(qw, d)], wqkv_sem.at[1]),
                local(wv_hbm.at[lay], wqkv_v.at[:, pl.ds(qw + d, d)], wqkv_sem.at[2]))

    def chunk_copy(step, which):
        lay = step // n_chunks
        col = pl.multiple_of(jnp.minimum((step % n_chunks) * CHUNK, ff - CHUNK), d)
        slot = step % SLOTS
        if which == 2:
            return local(wd_hbm.at[lay, pl.ds(col, CHUNK), :], wd_v.at[slot], slot_sem.at[slot, 2])
        src, dst = ((wg_hbm, wg_v), (wu_hbm, wu_v))[which]
        return local(src.at[lay, :, pl.ds(col, CHUNK)], dst.at[slot], slot_sem.at[slot, which])

    x_copy = local(x_hbm, x_v, in_sem.at[0])
    x_copy.start()
    for copy in qkv_copies(0):
        copy.start()
    barrier = pltpu.get_barrier_semaphore()

    def greet(i, carry):
        pl.semaphore_signal(barrier, inc=1, device_id={'sp': lax.rem(me + i, sp)}, device_id_type=MESH)
        return carry
    lax.fori_loop(1, sp, greet, 0)
    pl.semaphore_signal(barrier, inc=1, device_id=partner, device_id_type=MESH)

    lane = iota((1, d), 1)
    sign = jnp.where(lane < d // 2, -1.0, 1.0).astype(F32)
    freq = freq_ref[...]
    brow = iota((n_batch, d), 0)

    def place(b, acc):
        return jnp.where(brow == b, len_ref[b], acc)
    pos_b = lax.fori_loop(0, n_batch, place, jnp.zeros((n_batch, d), jnp.int32))
    angles = jnp.concatenate([(pos_b + s).astype(F32) * freq for s in range(n_steps)], axis=0)
    cos_t = jnp.cos(angles)
    sin_t = jnp.sin(angles) * sign
    row16 = iota((16, d), 0)
    my_pos = len_ref[me // 2] + 2 * lax.rem(me, 2) + row16 // 8
    my_angles = my_pos.astype(F32) * freq
    my_cos = jnp.cos(my_angles)
    my_sin = jnp.sin(my_angles) * sign

    def rope(v, c, s):
        return v * c + pltpu.roll(v, d // 2, 1) * s

    def rounded(v):
        return v.astype(BF16).astype(F32)

    x_copy.wait()
    xn_v[...] = norm(x_v[...].astype(F32), ga_ref[pl.ds(0, 1), :].astype(F32))
    for copy in qkv_copies(0):
        copy.wait()
    for lay in range(2):
        local(kc_hbm.at[lay], kc_v.at[lay], cache_sem.at[lay]).start()
        local(vc_hbm.at[lay], vc_v.at[lay], cache_sem.at[2 + lay]).start()
    wo_copy = local(wo_hbm.at[0], wo_v, wo_sem.at[0])
    wo_copy.start()

    def prefetch(step, carry):
        for which in range(3):
            chunk_copy(step, which).start()
        return carry
    lax.fori_loop(0, SLOTS, prefetch, 0)

    xn = xn_v[...]
    for pair in range(heads // 2):
        both = dot(xn, wqkv_v[:, pair * 256:pair * 256 + 256])
        for g in (2 * pair, 2 * pair + 1):
            off = (g % 2) * d
            q = rounded(rope(both[:, off:off + d], cos_t, sin_t))
            for s in range(n_steps):
                q0_v[pl.ds(s * heads + g, n_batch, stride=n_steps * heads), :] = q[s * n_batch:(s + 1) * n_batch]
    both = dot(xn, wqkv_v[:, qw:qw + 256])
    k0_v[...] = rounded(rope(both[:, :d], cos_t, sin_t))
    v0_v[...] = rounded(both[:, d:])
    for copy in qkv_copies(1):
        copy.start()

    own_row = (2 * lax.rem(me, 2) + iota((16, n_tok), 0) // 8) * n_batch + me // 2
    pick = jnp.where(iota((16, n_tok), 1) == own_row, 1.0, 0.0).astype(BF16)
    u = dot(pick, x_v[...])

    pos_row = iota((32, d), 1) * sp + me - iota((32, d), 0) // heads
    lane32 = iota((32, d), 1)
    slot_rows = iota((d, d), 0).astype(F32).astype(BF16)

    def attention(lay, q_ref, new_rows):
        def group(step, stat):
            for uu in range(UNROLL):
                b = lax.rem(me // 2 + step * UNROLL + uu, n_batch)
                length = len_ref[b]
                ahead = lax.rem(me - length + 1024 * sp, sp)
                slot = jnp.where(ahead < n_steps, (length + ahead) // sp, -1)
                hit = slot_rows == jnp.full((d, d), slot.astype(F32)).astype(BF16)
                k_row, v_row = new_rows(b, jnp.minimum(ahead, n_steps - 1))
                k_new = jnp.where(hit, jnp.broadcast_to(k_row, (d, d)).astype(BF16), kc_v[lay, b])
                v_new = jnp.where(hit, jnp.broadcast_to(v_row, (d, d)).astype(BF16), vc_v[lay, b])
                kc_v[lay, b] = k_new
                vc_v[lay, b] = v_new
                rows = pl.ds(pl.multiple_of(b * 32, 32), 32)
                q = q_ref[rows, :].astype(BF16)
                s = lax.dot_general(q, k_new, (((1,), (1,)), ((), ())), preferred_element_type=F32) * (d ** -0.5)
                s = jnp.where(pos_row <= length, s, -1e30)
                m = jnp.max(s, axis=-1, keepdims=True)
                w = jnp.exp(s - m)
                l = jnp.sum(w, axis=-1, keepdims=True)
                o_send[rows, :] = dot(w.astype(BF16), v_new)
                stat = jnp.where(lane32 == b, m, jnp.where(lane32 == 64 + b, l, stat))
            for uu in range(2 * UNROLL):
                dest = lax.rem(2 * (me // 2 + step * UNROLL) + uu, sp)

                @pl.when(dest != me)
                def _():
                    o_copy(lay, dest).start()
            return stat

        stat = lax.fori_loop(0, n_batch // UNROLL, group, jnp.zeros((32, d), F32))
        stat_t = jnp.transpose(jnp.concatenate([stat, jnp.zeros((d - 32, d), F32)], axis=0))
        st_send[:, 0, :] = jnp.where(lane32 < 32, stat_t[0:32], pltpu.roll(stat_t[64:96], 32, 1))

        def send_stat(i, carry):
            dest = lax.rem(me + i, sp)
            remote(st_send.at[dest // 2], st_recv.at[lay, me], st_ssem.at[lay], st_rsem.at[lay], {'sp': dest}).start()
            return carry
        lax.fori_loop(1, sp, send_stat, 0)
        mine = pl.ds(pl.multiple_of(me * 16, 16), 16)
        o_recv[lay, mine, :] = o_send[mine, :]
        st_recv[lay, me] = st_send[me // 2]
        local(kc_v.at[lay], ko_hbm.at[lay], out_sem.at[lay]).start()
        local(vc_v.at[lay], vo_hbm.at[lay], out_sem.at[2 + lay]).start()

        most = pl.ds(0, last * 16)
        remote(st_recv.at[lay, pl.ds(0, last)], st_recv.at[lay, pl.ds(0, last)], st_ssem.at[lay], st_rsem.at[lay], partner).wait_recv()
        stats = st_recv[lay, :, 0, :]
        top = jnp.max(stats, axis=0, keepdims=True)
        scale = jnp.exp(stats - top)
        denom = jnp.sum(pltpu.roll(scale, 32, 1) * stats, axis=0, keepdims=True)
        denom = pltpu.roll(jnp.broadcast_to(denom, (8, d)), d - 32, 1)
        tr_v[...] = jnp.transpose(jnp.concatenate([scale, denom, jnp.zeros((d - sp - 8, d), F32)], axis=0))
        factors = tr_v[pl.ds(pl.multiple_of(lax.rem(me, 2) * 16, 16), 16), :]
        remote(o_recv.at[lay, most], o_recv.at[lay, most], o_ssem.at[lay], o_rsem.at[lay], partner).wait_recv()
        merged = jnp.zeros((16, d), F32)
        for i in range(sp):
            merged = merged + factors[:, i:i + 1] * o_recv[lay, i * 16:i * 16 + 16, :]
        at_v[...] = merged / factors[:, sp:sp + 1]
        remote(o_send.at[most], o_send.at[most], o_ssem.at[lay], o_rsem.at[lay], partner).wait_send()
        remote(st_recv.at[lay, pl.ds(0, last)], st_recv.at[lay, pl.ds(0, last)], st_ssem.at[lay], st_rsem.at[lay], partner).wait_send()
        cols = []
        for g in range(heads):
            cols.append(jnp.concatenate([jnp.broadcast_to(at_v[g:g + 1, :], (8, d)), jnp.broadcast_to(at_v[8 + g:9 + g, :], (8, d))], axis=0))
        return jnp.concatenate(cols, axis=1).astype(BF16)

    def o_copy(lay, dest):
        return remote(o_send.at[pl.ds(pl.multiple_of(dest * 16, 16), 16)], o_recv.at[lay, pl.ds(pl.multiple_of(me * 16, 16), 16)],
                      o_ssem.at[lay], o_rsem.at[lay], {'sp': dest})

    def add_cores(i, part):
        x_send[i] = part
        copy = remote(x_send.at[i], x_recv.at[i], x_ssem.at[i], x_rsem.at[i], partner)
        copy.start()
        copy.wait()
        return part + x_recv[i]

    def mlp(lay, h):
        lane_c = iota((16, CHUNK), 1)

        def act(j):
            step = lay * n_chunks + j
            chunk_copy(step, 0).wait()
            chunk_copy(step, 1).wait()
            slot = step % SLOTS
            gate = dot(h, wg_v[slot])
            up = dot(h, wu_v[slot])
            a = gate * jax.nn.sigmoid(gate) * up
            return jnp.where(lane_c >= j * CHUNK - jnp.minimum(j * CHUNK, ff - CHUNK), a, 0.0).astype(BF16)

        def down(j, a):
            step = lay * n_chunks + j
            chunk_copy(step, 2).wait()
            return dot(a, wd_v[step % SLOTS])

        def refill(j):
            step = lay * n_chunks + j + SLOTS

            @pl.when(step < total)
            def _():
                for which in range(3):
                    chunk_copy(step, which).start()

        def body(j, a):
            nxt = act(j)
            acc_v[...] += down(j - 1, a)
            refill(j - 1)
            return nxt

        a = act(0)
        acc_v[...] = jnp.zeros_like(acc_v)
        a = lax.fori_loop(1, n_chunks, body, a)
        out = acc_v[...] + down(n_chunks - 1, a)
        refill(n_chunks - 1)
        return out

    def finish_layer(lay, u, attn):
        local(wo_hbm.at[lay], wo_v, wo_sem.at[0]).wait()
        u = rounded(u + add_cores(2 * lay, dot(attn, wo_v[...])))
        if lay == 0:
            local(wo_hbm.at[1], wo_v, wo_sem.at[0]).start()
        h = norm(u, gm_ref[pl.ds(lay, 1), :].astype(F32))
        return rounded(u + add_cores(2 * lay + 1, mlp(lay, h)))

    def send_all(send):
        def body(i, carry):
            dest = 0
            for unit in (side * side, side, 1):
                dest = dest + lax.rem(me // unit + i // unit + side // 2, side) * unit

            @pl.when(dest != me)
            def _():
                send(dest)
            return carry
        lax.fori_loop(0, sp, body, 0)

    def wait_cache(lay):
        local(kc_hbm.at[lay], kc_v.at[lay], cache_sem.at[lay]).wait()
        local(vc_hbm.at[lay], vc_v.at[lay], cache_sem.at[2 + lay]).wait()

    wait_cache(0)
    pl.semaphore_wait(barrier, sp)

    def rows0(b, ahead):
        return k0_v[pl.ds(ahead * n_batch + b, 1), :], v0_v[pl.ds(ahead * n_batch + b, 1), :]

    def rows1(b, ahead):
        chip = 2 * b + ahead // 2
        return kv_recv[chip, pl.ds(lax.rem(ahead, 2), 1), :], kv_recv[chip, pl.ds(2 + lax.rem(ahead, 2), 1), :]

    u = finish_layer(0, u, attention(0, q0_v, rows0))

    h = norm(u, ga_ref[pl.ds(1, 1), :].astype(F32))
    for copy in qkv_copies(1):
        copy.wait()
    sub = row16 % 8
    q = jnp.zeros((16, d), F32)
    for pair in range(heads // 2):
        both = dot(h, wqkv_v[:, pair * 256:pair * 256 + 256])
        q = jnp.where(sub == 2 * pair, both[:, :d], jnp.where(sub == 2 * pair + 1, both[:, d:], q))
    both = dot(h, wqkv_v[:, qw:qw + 256])
    q_send[...] = rounded(rope(q, my_cos, my_sin))
    k = rounded(rope(both[:, :d], my_cos, my_sin))
    v = rounded(both[:, d:])
    sub8 = iota((8, d), 0)
    kv = jnp.where(sub8 == 0, k[:8], jnp.where(sub8 == 1, k[8:], jnp.where(sub8 == 2, v[:8], v[8:])))
    kv_send[...] = kv[:4]
    mine = pl.ds(pl.multiple_of(me * 16, 16), 16)

    def send_qkv(dest):
        remote(kv_send, kv_recv.at[me], ag_ssem.at[1], ag_rsem.at[1], {'sp': dest}).start()
        remote(q_send, q_recv.at[mine], ag_ssem.at[0], ag_rsem.at[0], {'sp': dest}).start()
    send_all(send_qkv)
    q_recv[mine, :] = q_send[...]
    kv_recv[me] = kv_send[...]
    most = pl.ds(0, last * 16)
    wait_cache(1)
    for ref, sem in ((q_recv.at[most], 0), (kv_recv.at[pl.ds(0, last)], 1)):
        both_ways = remote(ref, ref, ag_ssem.at[sem], ag_rsem.at[sem], partner)
        both_ways.wait_recv()
        both_ways.wait_send()

    u = finish_layer(1, u, attention(1, q_recv, rows1))

    acc_v[...] = u
    half = width // 2
    msg = jnp.zeros((16, d), F32)
    for cg in range(8):
        msg = jnp.where(sub == cg, acc_v[:, pl.ds(pl.multiple_of(core * half + cg * d, d), d)], msg)
    h_send[...] = msg

    def send_hidden(dest):
        remote(h_send, h_recv.at[mine], ag_ssem.at[2], ag_rsem.at[2], {'sp': dest}).start()
    send_all(send_hidden)
    h_recv[mine, :] = h_send[...]
    both_ways = remote(h_recv.at[most], h_recv.at[most], ag_ssem.at[2], ag_rsem.at[2], partner)
    both_ways.wait_recv()
    both_ways.wait_send()
    swap = remote(h_recv, h_other, ag_ssem.at[3], ag_rsem.at[3], partner)
    swap.start()

    def spread(ref, which):
        for s in range(n_steps):
            for cg in range(8):
                rows = ref[pl.ds(s * 8 + cg, n_batch, stride=n_steps * 8), :]
                out_v[s * n_batch:(s + 1) * n_batch, pl.ds(pl.multiple_of(which * half + cg * d, d), d)] = rows.astype(BF16)
    spread(h_recv, core)
    swap.wait()
    spread(h_other, 1 - core)
    done = local(out_v, hid_hbm, in_sem.at[1])
    done.start()
    for lay in range(2):
        local(kc_v.at[lay], ko_hbm.at[lay], out_sem.at[lay]).wait()
        local(vc_v.at[lay], vo_hbm.at[lay], out_sem.at[2 + lay]).wait()
    done.wait()


def solution(mesh):
    sp = mesh.shape['sp']
    side = round(sp ** (1 / 3))

    def local_fn(tok_emb, lengths, key_cache, val_cache, gain_attn, gain_mlp, w_query, w_key, w_value, w_out, w_gate, w_up, w_down):
        n_steps, n_batch, width = tok_emb.shape
        n_layers, _, loc_len, _, d = key_cache.shape
        n_tok = n_steps * n_batch
        cache_shape = (n_layers, n_batch, loc_len, d)
        inv_freq = 1.0 / (ROPE_BASE ** (jnp.arange(d // 2).astype(F32) * 2.0 / d))
        freq = jnp.concatenate([inv_freq, inv_freq])[None, :]
        qw = w_query.shape[2]
        vmem = pltpu.VMEM
        dma = pltpu.SemaphoreType.DMA
        in_vmem = pl.BlockSpec(memory_space=pltpu.VMEM)
        in_any = pl.BlockSpec(memory_space=pl.ANY)
        outs = pl.pallas_call(
            functools.partial(kernel, sp, n_steps, n_batch, side),
            out_shape=(jax.ShapeDtypeStruct((n_tok, width), BF16), jax.ShapeDtypeStruct(cache_shape, BF16), jax.ShapeDtypeStruct(cache_shape, BF16)),
            in_specs=[pl.BlockSpec(memory_space=pltpu.SMEM)] + [in_vmem] * 3 + [in_any] * 10,
            out_specs=(in_any,) * 3,
            scratch_shapes=[
                vmem((n_tok, width), BF16), vmem((n_tok, width), BF16), vmem((width, qw + 2 * d), BF16), vmem((qw, width), BF16),
                vmem(cache_shape, BF16), vmem(cache_shape, BF16),
                vmem((SLOTS, width, CHUNK), BF16), vmem((SLOTS, width, CHUNK), BF16), vmem((SLOTS, CHUNK, width), BF16),
                vmem((sp * 16, d), F32), vmem((n_tok, d), F32), vmem((n_tok, d), F32),
                vmem((sp * 16, d), F32), vmem((sp, 4, d), F32),
                vmem((sp * 16, d), F32), vmem((2, sp * 16, d), F32), vmem((32, 1, d), F32), vmem((2, sp, 1, d), F32),
                vmem((4, 16, width), F32), vmem((4, 16, width), F32), vmem((16, width), F32),
                vmem((16, d), F32), vmem((4, d), F32), vmem((16, d), F32),
                vmem((sp * 16, d), F32), vmem((sp * 16, d), F32), vmem((n_tok, width), BF16), vmem((d, d), F32), vmem((16, d), F32),
                dma((2,)), dma((4,)), dma((4,)), dma((3,)), dma((1,)), dma((SLOTS, 3)),
                dma((2,)), dma((2,)), dma((2,)), dma((2,)), dma((4,)), dma((4,)), dma((4,)), dma((4,)),
            ],
            compiler_params=pltpu.CompilerParams(collective_id=0, has_side_effects=True, vmem_limit_bytes=67043328),
            name='decode',
        )(lengths, freq, gain_attn, gain_mlp, tok_emb.reshape(n_tok, width), key_cache.reshape(cache_shape), val_cache.reshape(cache_shape),
          w_query, w_key, w_value, w_out, w_gate, w_up, w_down)
        hidden, new_keys, new_vals = outs
        return hidden.reshape(n_steps, n_batch, width), new_keys.reshape(key_cache.shape), new_vals.reshape(val_cache.shape)

    cache_spec = P(None, 'dp', 'sp', 'tp', None)
    col_spec = P(None, None, 'tp')
    row_spec = P(None, 'tp', None)
    emb_spec = P(None, 'dp', None)
    return jax.shard_map(local_fn, mesh=mesh, in_specs=(emb_spec, P('dp'), cache_spec, cache_spec, P(), P(), col_spec, col_spec, col_spec, row_spec, col_spec, col_spec, row_spec), out_specs=(emb_spec, cache_spec, cache_spec), check_vma=False)
```

```python
import functools

import jax
import jax.numpy as jnp
import numpy as np
from jax import lax
from jax.experimental import pallas as pl
from jax.experimental.pallas import tpu as pltpu
from jax.sharding import PartitionSpec as P

EPS = 1e-5
ROPE_BASE = 500000.0
CHUNK = 512
SLOTS = 7
UNROLL = 8
F32 = jnp.float32
BF16 = jnp.bfloat16
MESH = pl.DeviceIdType.MESH


def dot(a, b):
    return jnp.dot(a, b, preferred_element_type=F32)


def norm(u, gain):
    inv = lax.rsqrt(jnp.mean(u * u, axis=-1, keepdims=True) + EPS)
    return (u * inv * gain).astype(BF16)


def iota(shape, dim):
    return lax.broadcasted_iota(jnp.int32, shape, dim)


def kernel(sp, n_steps, n_batch, side,
           len_ref, freq_ref, ga_ref, gm_ref, x_hbm, kc_hbm, vc_hbm, wq_hbm, wk_hbm, wv_hbm, wo_hbm, wg_hbm, wu_hbm, wd_hbm,
           hid_hbm, ko_hbm, vo_hbm,
           x_v, xn_v, wqkv_v, wo_v, kc_v, vc_v, wg_v, wu_v, wd_v, q0_v, k0_v, v0_v,
           qkv_recv, o_send, o_recv, st_send, st_recv, x_send, x_recv, acc_v, qkv_send, h_send,
           h_recv, h_other, tr_v, at_v,
           in_sem, cache_sem, out_sem, wqkv_sem, wo_sem, slot_sem,
           o_ssem, o_rsem, st_ssem, st_rsem, x_ssem, x_rsem, ag_ssem, qkv_rsem, h_rsem, sw_ssem, sw_rsem):
    me = lax.axis_index('sp')
    core = lax.axis_index('tp')
    n_tok = n_steps * n_batch
    width = x_v.shape[1]
    d = 128
    ff = wg_hbm.shape[2]
    heads = wq_hbm.shape[2] // d
    qw = heads * d
    n_chunks = -(-ff // CHUNK)
    total = 2 * n_chunks
    last = sp - 1
    partner = {'tp': 1 - core}
    plane = side * side
    my_plane = me // plane
    out_v = x_v

    def local(src, dst, sem):
        return pltpu.make_async_copy(src, dst, sem)

    def remote(src, dst, ssem, rsem, dev):
        return pltpu.make_async_remote_copy(src_ref=src, dst_ref=dst, send_sem=ssem, recv_sem=rsem, device_id=dev, device_id_type=MESH)

    def qkv_copies(lay):
        copies = [local(wq_hbm.at[lay, :, pl.ds(i * 256, 256)], wqkv_v.at[:, pl.ds(i * 256, 256)], wqkv_sem.at[i]) for i in range(qw // 256)]
        copies.append(local(wk_hbm.at[lay], wqkv_v.at[:, pl.ds(qw, d)], wqkv_sem.at[qw // 256]))
        copies.append(local(wv_hbm.at[lay], wqkv_v.at[:, pl.ds(qw + d, d)], wqkv_sem.at[qw // 256 + 1]))
        return copies

    def each_other(send):
        many = 9 if last % 9 == 0 else 1

        def body(i, carry):
            for j in range(many):
                send(lax.rem(me + 1 + lax.rem(i * many + j + sp // 2 - 1, last), sp))
            return carry
        lax.fori_loop(0, last // many, body, 0)

    def chunk_copy(step, which):
        lay = step // n_chunks
        col = pl.multiple_of(jnp.minimum((step % n_chunks) * CHUNK, ff - CHUNK), d)
        slot = step % SLOTS
        if which == 2:
            return local(wd_hbm.at[lay, pl.ds(col, CHUNK), :], wd_v.at[slot], slot_sem.at[slot, 2])
        src, dst = ((wg_hbm, wg_v), (wu_hbm, wu_v))[which]
        return local(src.at[lay, :, pl.ds(col, CHUNK)], dst.at[slot], slot_sem.at[slot, which])

    x_copy = local(x_hbm, x_v, in_sem.at[0])
    x_copy.start()
    for copy in qkv_copies(0):
        copy.start()
    barrier = pltpu.get_barrier_semaphore()
    each_other(lambda dest: pl.semaphore_signal(barrier, inc=1, device_id={'sp': dest}, device_id_type=MESH))
    pl.semaphore_signal(barrier, inc=1, device_id=partner, device_id_type=MESH)

    lane = iota((1, d), 1)
    sign = jnp.where(lane < d // 2, -1.0, 1.0).astype(F32)
    freq = freq_ref[...]
    brow = iota((n_batch, d), 0)

    def place(b, acc):
        return jnp.where(brow == b, len_ref[b], acc)
    pos_b = lax.fori_loop(0, n_batch, place, jnp.zeros((n_batch, d), jnp.int32))
    angles = jnp.concatenate([(pos_b + s).astype(F32) * freq for s in range(n_steps)], axis=0)
    cos_t = jnp.cos(angles)
    sin_t = jnp.sin(angles) * sign
    row16 = iota((16, d), 0)
    my_pos = len_ref[me // 2] + 2 * lax.rem(me, 2) + row16 // 8
    my_angles = my_pos.astype(F32) * freq
    my_cos = jnp.cos(my_angles)
    my_sin = jnp.sin(my_angles) * sign

    def rope(v, c, s):
        return v * c + pltpu.roll(v, d // 2, 1) * s

    def rounded(v):
        return v.astype(BF16).astype(F32)

    x_copy.wait()
    xn_v[...] = norm(x_v[...].astype(F32), ga_ref[pl.ds(0, 1), :].astype(F32))
    for lay in range(2):
        local(kc_hbm.at[lay], kc_v.at[lay], cache_sem.at[lay]).start()
        local(vc_hbm.at[lay], vc_v.at[lay], cache_sem.at[2 + lay]).start()
    wo_copy = local(wo_hbm.at[0], wo_v, wo_sem.at[0])
    wo_copy.start()

    def prefetch(step, carry):
        for which in range(3):
            chunk_copy(step, which).start()
        return carry
    lax.fori_loop(0, SLOTS, prefetch, 0)

    xn = xn_v[...]
    waits = qkv_copies(0)
    for pair in range(heads // 2):
        waits[pair].wait()
        both = dot(xn, wqkv_v[:, pair * 256:pair * 256 + 256])
        for g in (2 * pair, 2 * pair + 1):
            off = (g % 2) * d
            q = rounded(rope(both[:, off:off + d], cos_t, sin_t))
            for s in range(n_steps):
                q0_v[pl.ds(s * heads + g, n_batch, stride=n_steps * heads), :] = q[s * n_batch:(s + 1) * n_batch]
    waits[-2].wait()
    waits[-1].wait()
    both = dot(xn, wqkv_v[:, qw:qw + 256])
    k0_v[...] = rounded(rope(both[:, :d], cos_t, sin_t))
    v0_v[...] = rounded(both[:, d:])
    for copy in qkv_copies(1):
        copy.start()

    own_row = (2 * lax.rem(me, 2) + iota((16, n_tok), 0) // 8) * n_batch + me // 2
    pick = jnp.where(iota((16, n_tok), 1) == own_row, 1.0, 0.0).astype(BF16)
    u = dot(pick, x_v[...])

    pos_row = iota((32, d), 1) * sp + me - iota((32, d), 0) // heads
    lane32 = iota((32, d), 1)
    slot_rows = iota((d, d), 0).astype(F32).astype(BF16)

    def attention(lay, arrive, queries, new_rows):
        def group(step, stat):
            first = lax.rem(my_plane + step, side) * UNROLL
            turn = lax.rem(me, plane) // 2
            arrive(step)
            for uu in range(UNROLL):
                b = first + lax.rem(turn + uu, UNROLL)
                length = len_ref[b]
                ahead = lax.rem(me - length + 1024 * sp, sp)
                slot = jnp.where(ahead < n_steps, (length + ahead) // sp, -1)
                hit = slot_rows == jnp.full((d, d), slot.astype(F32)).astype(BF16)
                k_row, v_row = new_rows(b, jnp.minimum(ahead, n_steps - 1))
                k_new = jnp.where(hit, jnp.broadcast_to(k_row, (d, d)).astype(BF16), kc_v[lay, b])
                v_new = jnp.where(hit, jnp.broadcast_to(v_row, (d, d)).astype(BF16), vc_v[lay, b])
                kc_v[lay, b] = k_new
                vc_v[lay, b] = v_new
                rows = pl.ds(pl.multiple_of(b * 32, 32), 32)
                q = queries(b).astype(BF16)
                s = lax.dot_general(q, k_new, (((1,), (1,)), ((), ())), preferred_element_type=F32) * (d ** -0.5)
                s = jnp.where(pos_row <= length, s, -1e30)
                m = jnp.max(s, axis=-1, keepdims=True)
                w = jnp.exp(s - m)
                l = jnp.sum(w, axis=-1, keepdims=True)
                o_send[rows, :] = dot(w.astype(BF16), v_new)
                stat = jnp.where(lane32 == b, m, jnp.where(lane32 == 64 + b, l, stat))
            for uu in range(2 * UNROLL):
                dest = 2 * first + lax.rem(2 * turn + uu, 2 * UNROLL)

                @pl.when(dest != me)
                def _():
                    o_copy(lay, dest).start()
            return stat

        stat = lax.fori_loop(0, n_batch // UNROLL, group, jnp.zeros((32, d), F32))
        stat_t = jnp.transpose(jnp.concatenate([stat, jnp.zeros((d - 32, d), F32)], axis=0))
        st_send[:, 0, :] = jnp.where(lane32 < 32, stat_t[0:32], pltpu.roll(stat_t[64:96], 32, 1))

        each_other(lambda dest: remote(st_send.at[dest // 2], st_recv.at[lay, me], st_ssem.at[lay], st_rsem.at[lay], {'sp': dest}).start())
        mine = pl.ds(pl.multiple_of(me * 16, 16), 16)
        o_recv[lay, mine, :] = o_send[mine, :]
        st_recv[lay, me] = st_send[me // 2]
        local(kc_v.at[lay], ko_hbm.at[lay], out_sem.at[lay]).start()
        local(vc_v.at[lay], vo_hbm.at[lay], out_sem.at[2 + lay]).start()

        most = pl.ds(0, last * 16)
        remote(st_recv.at[lay, pl.ds(0, last)], st_recv.at[lay, pl.ds(0, last)], st_ssem.at[lay], st_rsem.at[lay], partner).wait_recv()
        stats = st_recv[lay, :, 0, :]
        top = jnp.max(stats, axis=0, keepdims=True)
        scale = jnp.exp(stats - top)
        denom = jnp.sum(pltpu.roll(scale, 32, 1) * stats, axis=0, keepdims=True)
        denom = pltpu.roll(jnp.broadcast_to(denom, (8, d)), d - 32, 1)
        tr_v[...] = jnp.transpose(jnp.concatenate([scale, denom, jnp.zeros((d - sp - 8, d), F32)], axis=0))
        factors = tr_v[pl.ds(pl.multiple_of(lax.rem(me, 2) * 16, 16), 16), :]
        remote(o_recv.at[lay, most], o_recv.at[lay, most], o_ssem.at[lay], o_rsem.at[lay], partner).wait_recv()
        merged = jnp.zeros((16, d), F32)
        for i in range(sp):
            merged = merged + factors[:, i:i + 1] * o_recv[lay, i * 16:i * 16 + 16, :]
        at_v[...] = merged / factors[:, sp:sp + 1]
        remote(o_send.at[most], o_send.at[most], o_ssem.at[lay], o_rsem.at[lay], partner).wait_send()
        remote(st_recv.at[lay, pl.ds(0, last)], st_recv.at[lay, pl.ds(0, last)], st_ssem.at[lay], st_rsem.at[lay], partner).wait_send()
        cols = []
        for g in range(heads):
            cols.append(jnp.concatenate([jnp.broadcast_to(at_v[g:g + 1, :], (8, d)), jnp.broadcast_to(at_v[8 + g:9 + g, :], (8, d))], axis=0))
        return jnp.concatenate(cols, axis=1).astype(BF16)

    def o_copy(lay, dest):
        return remote(o_send.at[pl.ds(pl.multiple_of(dest * 16, 16), 16)], o_recv.at[lay, pl.ds(pl.multiple_of(me * 16, 16), 16)],
                      o_ssem.at[lay], o_rsem.at[lay], {'sp': dest})

    def add_cores(i, part):
        x_send[i] = part
        copy = remote(x_send.at[i], x_recv.at[i], x_ssem.at[i], x_rsem.at[i], partner)
        copy.start()
        copy.wait()
        return part + x_recv[i]

    def mlp(lay, h):
        lane_c = iota((16, CHUNK), 1)

        def act(j):
            step = lay * n_chunks + j
            chunk_copy(step, 0).wait()
            chunk_copy(step, 1).wait()
            slot = step % SLOTS
            gate = dot(h, wg_v[slot])
            up = dot(h, wu_v[slot])
            a = gate * jax.nn.sigmoid(gate) * up
            return jnp.where(lane_c >= j * CHUNK - jnp.minimum(j * CHUNK, ff - CHUNK), a, 0.0).astype(BF16)

        def down(j, a):
            step = lay * n_chunks + j
            chunk_copy(step, 2).wait()
            return dot(a, wd_v[step % SLOTS])

        def refill(j):
            step = lay * n_chunks + j + SLOTS

            @pl.when(step < total)
            def _():
                for which in range(3):
                    chunk_copy(step, which).start()

        def body(j, a):
            nxt = act(j)
            acc_v[...] += down(j - 1, a)
            refill(j - 1)
            return nxt

        a = act(0)
        acc_v[...] = jnp.zeros_like(acc_v)
        a = lax.fori_loop(1, n_chunks, body, a)
        out = acc_v[...] + down(n_chunks - 1, a)
        refill(n_chunks - 1)
        return out

    def finish_layer(lay, u, attn):
        local(wo_hbm.at[lay], wo_v, wo_sem.at[0]).wait()
        u = rounded(u + add_cores(2 * lay, dot(attn, wo_v[...])))
        if lay == 0:
            local(wo_hbm.at[1], wo_v, wo_sem.at[0]).start()
        h = norm(u, gm_ref[pl.ds(lay, 1), :].astype(F32))
        return rounded(u + add_cores(2 * lay + 1, mlp(lay, h)))

    def wait_cache(lay):
        local(kc_hbm.at[lay], kc_v.at[lay], cache_sem.at[lay]).wait()
        local(vc_hbm.at[lay], vc_v.at[lay], cache_sem.at[2 + lay]).wait()

    wait_cache(0)
    pl.semaphore_wait(barrier, sp)

    def queries0(b):
        return q0_v[pl.ds(pl.multiple_of(b * 32, 32), 32), :]

    def rows0(b, ahead):
        return k0_v[pl.ds(ahead * n_batch + b, 1), :], v0_v[pl.ds(ahead * n_batch + b, 1), :]

    def queries1(b):
        return jnp.concatenate([qkv_recv[2 * b, 0:16, :], qkv_recv[2 * b + 1, 0:16, :]], axis=0)

    def rows1(b, ahead):
        kv = jnp.where(ahead >= 2, qkv_recv[2 * b + 1, 16:20, :], qkv_recv[2 * b, 16:20, :])
        odd = lax.rem(ahead, 2) == 1
        return jnp.where(odd, kv[1:2], kv[0:1]), jnp.where(odd, kv[3:4], kv[2:3])

    def wait_plane(step, part, ssem, rsem):
        which = lax.rem(my_plane + step, side)

        @pl.when(step == 0)
        def _():
            remote(part(plane - 1), part(plane - 1), ssem, rsem.at[which], partner).wait_recv()

        @pl.when(step != 0)
        def _():
            remote(part(plane), part(plane), ssem, rsem.at[which], partner).wait_recv()

    u = finish_layer(0, u, attention(0, lambda step: None, queries0, rows0))

    h = norm(u, ga_ref[pl.ds(1, 1), :].astype(F32))
    waits = qkv_copies(1)
    for copy in waits:
        copy.wait()
    sub = row16 % 8
    q = jnp.zeros((16, d), F32)
    for pair in range(heads // 2):
        both = dot(h, wqkv_v[:, pair * 256:pair * 256 + 256])
        q = jnp.where(sub == 2 * pair, both[:, :d], jnp.where(sub == 2 * pair + 1, both[:, d:], q))
    both = dot(h, wqkv_v[:, qw:qw + 256])
    qkv_send[0:16, :] = rounded(rope(q, my_cos, my_sin))
    k = rounded(rope(both[:, :d], my_cos, my_sin))
    v = rounded(both[:, d:])
    sub8 = iota((8, d), 0)
    kv = jnp.where(sub8 == 0, k[:8], jnp.where(sub8 == 1, k[8:], jnp.where(sub8 == 2, v[:8], v[8:])))
    qkv_send[16:20, :] = kv[:4]
    each_other(lambda dest: remote(qkv_send, qkv_recv.at[me], ag_ssem.at[0], qkv_rsem.at[my_plane], {'sp': dest}).start())
    qkv_recv[me] = qkv_send[...]
    wait_cache(1)

    def arrive(step):
        wait_plane(step, lambda n: qkv_recv.at[pl.ds(0, n)], ag_ssem.at[0], qkv_rsem)

    u = finish_layer(1, u, attention(1, arrive, queries1, rows1))
    remote(qkv_recv.at[pl.ds(0, last)], qkv_recv.at[pl.ds(0, last)], ag_ssem.at[0], qkv_rsem.at[0], partner).wait_send()

    acc_v[...] = u
    half = width // 2
    msg = jnp.zeros((16, d), F32)
    for cg in range(8):
        msg = jnp.where(sub == cg, acc_v[:, pl.ds(pl.multiple_of(core * half + cg * d, d), d)], msg)
    h_send[...] = msg

    mine = pl.ds(pl.multiple_of(me * 16, 16), 16)
    each_other(lambda dest: remote(h_send, h_recv.at[mine], ag_ssem.at[1], h_rsem.at[my_plane], {'sp': dest}).start())
    h_recv[mine, :] = h_send[...]

    def swap(step):
        rows = pl.ds(pl.multiple_of(lax.rem(my_plane + step, side) * plane * 16, plane * 16), plane * 16)
        return remote(h_recv.at[rows], h_other.at[rows], sw_ssem.at[step], sw_rsem.at[step], partner)
    for step in range(side):
        wait_plane(step, lambda n: h_recv.at[pl.ds(0, n * 16)], ag_ssem.at[1], h_rsem)
        swap(step).start()

    def spread(ref, which):
        for s in range(n_steps):
            for cg in range(8):
                rows = ref[pl.ds(s * 8 + cg, n_batch, stride=n_steps * 8), :]
                out_v[s * n_batch:(s + 1) * n_batch, pl.ds(pl.multiple_of(which * half + cg * d, d), d)] = rows.astype(BF16)
    spread(h_recv, core)
    for step in range(side):
        swap(step).wait()
    spread(h_other, 1 - core)
    done = local(out_v, hid_hbm, in_sem.at[1])
    done.start()
    most = pl.ds(0, last * 16)
    remote(h_recv.at[most], h_recv.at[most], ag_ssem.at[1], h_rsem.at[0], partner).wait_send()
    for lay in range(2):
        local(kc_v.at[lay], ko_hbm.at[lay], out_sem.at[lay]).wait()
        local(vc_v.at[lay], vo_hbm.at[lay], out_sem.at[2 + lay]).wait()
    done.wait()


def deliver_kernel(parts, *refs):
    n = len(parts)
    srcs, dsts, bufs, sems = refs[:n], refs[n:2 * n], refs[2 * n:3 * n], refs[3 * n]
    loads, stores = [], []
    for i, part in enumerate(parts):
        for j in range(srcs[i].shape[0] // part):
            rows = pl.ds(j * part, part)
            loads.append(pltpu.make_async_copy(srcs[i].at[rows], bufs[i].at[rows], sems.at[0, len(loads)]))
            stores.append(pltpu.make_async_copy(bufs[i].at[rows], dsts[i].at[rows], sems.at[1, len(stores)]))
    for load in loads:
        load.start()
    for load, store in zip(loads, stores):
        load.wait()
        store.start()
    for store in stores:
        store.wait()


def deliver(arrays):
    flat = [a.reshape(-1, a.shape[-1]) for a in arrays]
    parts = [max(a.shape[0] // 4, 16) if a.shape[0] > 1024 else a.shape[0] for a in flat]
    count = sum(a.shape[0] // part for a, part in zip(flat, parts))
    any_space = pl.BlockSpec(memory_space=pl.ANY)
    return pl.pallas_call(
        functools.partial(deliver_kernel, parts),
        out_shape=tuple(jax.ShapeDtypeStruct(a.shape, a.dtype) for a in flat),
        in_specs=[any_space] * len(flat),
        out_specs=(any_space,) * len(flat),
        scratch_shapes=[pltpu.VMEM(a.shape, a.dtype) for a in flat] + [pltpu.SemaphoreType.DMA((2, count))],
        compiler_params=pltpu.CompilerParams(vmem_limit_bytes=67043328),
        name='deliver',
    )(*flat)


def solution(mesh):
    sp = mesh.shape['sp']
    side = round(sp ** (1 / 3))

    def local_fn(tok_emb, lengths, key_cache, val_cache, gain_attn, gain_mlp, w_query, w_key, w_value, w_out, w_gate, w_up, w_down):
        n_steps, n_batch, width = tok_emb.shape
        n_layers, _, loc_len, _, d = key_cache.shape
        n_tok = n_steps * n_batch
        cache_shape = (n_layers, n_batch, loc_len, d)
        inv_freq = np.float32(1.0) / np.float32(ROPE_BASE) ** (np.arange(d // 2, dtype=np.float32) * np.float32(2.0) / np.float32(d))
        freq = jnp.asarray(np.concatenate([inv_freq, inv_freq])[None, :], F32)
        qw = w_query.shape[2]
        vmem = pltpu.VMEM
        dma = pltpu.SemaphoreType.DMA
        in_vmem = pl.BlockSpec(memory_space=pltpu.VMEM)
        in_any = pl.BlockSpec(memory_space=pl.ANY)
        outs = pl.pallas_call(
            functools.partial(kernel, sp, n_steps, n_batch, side),
            out_shape=(jax.ShapeDtypeStruct((n_tok, width), BF16), jax.ShapeDtypeStruct(cache_shape, BF16), jax.ShapeDtypeStruct(cache_shape, BF16)),
            in_specs=[pl.BlockSpec(memory_space=pltpu.SMEM)] + [in_vmem] * 3 + [in_any] * 10,
            out_specs=(in_any,) * 3,
            scratch_shapes=[
                vmem((n_tok, width), BF16), vmem((n_tok, width), BF16), vmem((width, qw + 2 * d), BF16), vmem((qw, width), BF16),
                vmem(cache_shape, BF16), vmem(cache_shape, BF16),
                vmem((SLOTS, width, CHUNK), BF16), vmem((SLOTS, width, CHUNK), BF16), vmem((SLOTS, CHUNK, width), BF16),
                vmem((sp * 16, d), F32), vmem((n_tok, d), F32), vmem((n_tok, d), F32),
                vmem((sp, 20, d), F32),
                vmem((sp * 16, d), F32), vmem((2, sp * 16, d), F32), vmem((32, 1, d), F32), vmem((2, sp, 1, d), F32),
                vmem((4, 16, width), F32), vmem((4, 16, width), F32), vmem((16, width), F32),
                vmem((20, d), F32), vmem((16, d), F32),
                vmem((sp * 16, d), F32), vmem((sp * 16, d), F32), vmem((d, d), F32), vmem((16, d), F32),
                dma((2,)), dma((4,)), dma((4,)), dma((qw // 256 + 2,)), dma((1,)), dma((SLOTS, 3)),
                dma((2,)), dma((2,)), dma((2,)), dma((2,)), dma((4,)), dma((4,)), dma((2,)), dma((side,)), dma((side,)), dma((side,)), dma((side,)),
            ],
            compiler_params=pltpu.CompilerParams(collective_id=0, has_side_effects=True, vmem_limit_bytes=67043328),
            name='decode',
        )(lengths, freq, gain_attn, gain_mlp, tok_emb.reshape(n_tok, width), key_cache.reshape(cache_shape), val_cache.reshape(cache_shape),
          w_query, w_key, w_value, w_out, w_gate, w_up, w_down)
        hidden, new_keys, new_vals = deliver(outs)
        return hidden.reshape(n_steps, n_batch, width), new_keys.reshape(key_cache.shape), new_vals.reshape(val_cache.shape)

    cache_spec = P(None, 'dp', 'sp', 'tp', None)
    col_spec = P(None, None, 'tp')
    row_spec = P(None, 'tp', None)
    emb_spec = P(None, 'dp', None)
    return jax.shard_map(local_fn, mesh=mesh, in_specs=(emb_spec, P('dp'), cache_spec, cache_spec, P(), P(), col_spec, col_spec, col_spec, row_spec, col_spec, col_spec, row_spec), out_specs=(emb_spec, cache_spec, cache_spec), check_vma=False)
```

```python
import functools

import jax
import jax.numpy as jnp
import numpy as np
from jax import lax
from jax.experimental import pallas as pl
from jax.experimental.pallas import tpu as pltpu
from jax.sharding import PartitionSpec as P

EPS = 1e-5
ROPE_BASE = 500000.0
TEAM = 4
PIECE = 512
UNROLL = 8
F32 = jnp.float32
BF16 = jnp.bfloat16
MESH = pl.DeviceIdType.MESH


def dot(a, b):
    return jnp.dot(a, b, preferred_element_type=F32)


def norm(u, gain):
    inv = lax.rsqrt(jnp.mean(u * u, axis=-1, keepdims=True) + EPS)
    return (u * inv * gain).astype(BF16)


def iota(shape, dim):
    return lax.broadcasted_iota(jnp.int32, shape, dim)


def kernel(sp, n_steps, n_batch, side,
           len_ref, freq_ref, ga_ref, gm_ref, x_hbm, kc_hbm, vc_hbm, wq_hbm, wk_hbm, wv_hbm, wo_hbm, wg_hbm, wu_hbm, wd_hbm,
           hid_hbm, ko_hbm, vo_hbm,
           x_v, xn_v, wqkv_v, wo_v, kc_v, vc_v, wg_v, wu_v, wd_v, q0_v, k0_v, v0_v,
           qkv_recv, o_send, o_recv, st_send, st_recv, a_send, a_recv, b_send, b_recv, rows_v, res_v, qkv_send, h_send,
           h_recv, h_other, tr_v, at_v,
           in_sem, cache_sem, out_sem, wqkv_sem, wo_sem, mlp_sem,
           o_ssem, o_rsem, st_ssem, st_rsem, a_ssem, a_rsem, b_ssem, b_rsem, ag_ssem, qkv_rsem, h_rsem, sw_ssem, sw_rsem):
    me = lax.axis_index('sp')
    core = lax.axis_index('tp')
    n_tok = n_steps * n_batch
    width = x_v.shape[1]
    d = 128
    ff = wg_hbm.shape[2]
    heads = wq_hbm.shape[2] // d
    qw = heads * d
    share = wg_v.shape[2]
    team = me // TEAM * TEAM
    rank = lax.rem(me, TEAM)
    col = pl.multiple_of(jnp.minimum(rank * share, ff - share), d)
    groups = width // d
    mine32 = 2 * groups
    last = sp - 1
    partner = {'tp': 1 - core}
    plane = side * side
    my_plane = me // plane
    out_v = x_v

    def local(src, dst, sem):
        return pltpu.make_async_copy(src, dst, sem)

    def remote(src, dst, ssem, rsem, dev):
        return pltpu.make_async_remote_copy(src_ref=src, dst_ref=dst, send_sem=ssem, recv_sem=rsem, device_id=dev, device_id_type=MESH)

    def qkv_copies(lay):
        copies = [local(wq_hbm.at[lay, :, pl.ds(i * 256, 256)], wqkv_v.at[:, pl.ds(i * 256, 256)], wqkv_sem.at[i]) for i in range(qw // 256)]
        copies.append(local(wk_hbm.at[lay], wqkv_v.at[:, pl.ds(qw, d)], wqkv_sem.at[qw // 256]))
        copies.append(local(wv_hbm.at[lay], wqkv_v.at[:, pl.ds(qw + d, d)], wqkv_sem.at[qw // 256 + 1]))
        return copies

    def each_other(send):
        many = 9 if last % 9 == 0 else 1

        def body(i, carry):
            for j in range(many):
                send(lax.rem(me + 1 + lax.rem(i * many + j + sp // 2 - 1, last), sp))
            return carry
        lax.fori_loop(0, last // many, body, 0)

    def mlp_copies(lay):
        return (local(wg_hbm.at[lay, :, pl.ds(col, share)], wg_v.at[lay], mlp_sem.at[lay, 0]),
                local(wu_hbm.at[lay, :, pl.ds(col, share)], wu_v.at[lay], mlp_sem.at[lay, 1]),
                local(wd_hbm.at[lay, pl.ds(col, share), :], wd_v.at[lay], mlp_sem.at[lay, 2]))

    x_copy = local(x_hbm, x_v, in_sem.at[0])
    x_copy.start()
    for copy in qkv_copies(0):
        copy.start()
    barrier = pltpu.get_barrier_semaphore()
    each_other(lambda dest: pl.semaphore_signal(barrier, inc=1, device_id={'sp': dest}, device_id_type=MESH))
    for j in range(TEAM):
        pl.semaphore_signal(barrier, inc=1, device_id={'sp': team + j, 'tp': 1 - core}, device_id_type=MESH)

    lane = iota((1, d), 1)
    sign = jnp.where(lane < d // 2, -1.0, 1.0).astype(F32)
    freq = freq_ref[...]
    brow = iota((n_batch, d), 0)

    def place(b, acc):
        return jnp.where(brow == b, len_ref[b], acc)
    pos_b = lax.fori_loop(0, n_batch, place, jnp.zeros((n_batch, d), jnp.int32))
    angles = jnp.concatenate([(pos_b + s).astype(F32) * freq for s in range(n_steps)], axis=0)
    cos_t = jnp.cos(angles)
    sin_t = jnp.sin(angles) * sign
    row16 = iota((16, d), 0)
    my_pos = len_ref[me // 2] + 2 * lax.rem(me, 2) + row16 // 8
    my_angles = my_pos.astype(F32) * freq
    my_cos = jnp.cos(my_angles)
    my_sin = jnp.sin(my_angles) * sign

    def rope(v, c, s):
        return v * c + pltpu.roll(v, d // 2, 1) * s

    def rounded(v):
        return v.astype(BF16).astype(F32)

    x_copy.wait()
    xn_v[...] = norm(x_v[...].astype(F32), ga_ref[pl.ds(0, 1), :].astype(F32))
    for lay in range(2):
        local(kc_hbm.at[lay], kc_v.at[lay], cache_sem.at[lay]).start()
        local(vc_hbm.at[lay], vc_v.at[lay], cache_sem.at[2 + lay]).start()
    wo_copy = local(wo_hbm.at[0], wo_v, wo_sem.at[0])
    wo_copy.start()

    for lay in range(2):
        for copy in mlp_copies(lay):
            copy.start()

    xn = xn_v[...]
    waits = qkv_copies(0)
    for pair in range(heads // 2):
        waits[pair].wait()
        both = dot(xn, wqkv_v[:, pair * 256:pair * 256 + 256])
        for g in (2 * pair, 2 * pair + 1):
            off = (g % 2) * d
            q = rounded(rope(both[:, off:off + d], cos_t, sin_t))
            for s in range(n_steps):
                q0_v[pl.ds(s * heads + g, n_batch, stride=n_steps * heads), :] = q[s * n_batch:(s + 1) * n_batch]
    waits[-2].wait()
    waits[-1].wait()
    both = dot(xn, wqkv_v[:, qw:qw + 256])
    k0_v[...] = rounded(rope(both[:, :d], cos_t, sin_t))
    v0_v[...] = rounded(both[:, d:])
    for copy in qkv_copies(1):
        copy.start()

    own_row = (2 * lax.rem(me, 2) + iota((16, n_tok), 0) // 8) * n_batch + me // 2
    pick = jnp.where(iota((16, n_tok), 1) == own_row, 1.0, 0.0).astype(BF16)
    u = dot(pick, x_v[...])

    pos_row = iota((32, d), 1) * sp + me - iota((32, d), 0) // heads
    lane32 = iota((32, d), 1)
    slot_rows = iota((d, d), 0).astype(F32).astype(BF16)

    def attention(lay, arrive, queries, new_rows):
        def group(step, stat):
            first = lax.rem(my_plane + step, side) * UNROLL
            turn = lax.rem(me, plane) // 2
            arrive(step)
            for uu in range(UNROLL):
                b = first + lax.rem(turn + uu, UNROLL)
                length = len_ref[b]
                ahead = lax.rem(me - length + 1024 * sp, sp)
                slot = jnp.where(ahead < n_steps, (length + ahead) // sp, -1)
                hit = slot_rows == jnp.full((d, d), slot.astype(F32)).astype(BF16)
                k_row, v_row = new_rows(b, jnp.minimum(ahead, n_steps - 1))
                k_new = jnp.where(hit, jnp.broadcast_to(k_row, (d, d)).astype(BF16), kc_v[lay, b])
                v_new = jnp.where(hit, jnp.broadcast_to(v_row, (d, d)).astype(BF16), vc_v[lay, b])
                kc_v[lay, b] = k_new
                vc_v[lay, b] = v_new
                rows = pl.ds(pl.multiple_of(b * 32, 32), 32)
                q = queries(b).astype(BF16)
                s = lax.dot_general(q, k_new, (((1,), (1,)), ((), ())), preferred_element_type=F32) * (d ** -0.5)
                s = jnp.where(pos_row <= length, s, -1e30)
                m = jnp.max(s, axis=-1, keepdims=True)
                w = jnp.exp(s - m)
                l = jnp.sum(w, axis=-1, keepdims=True)
                o_send[rows, :] = dot(w.astype(BF16), v_new)
                stat = jnp.where(lane32 == b, m, jnp.where(lane32 == 64 + b, l, stat))
            for uu in range(2 * UNROLL):
                dest = 2 * first + lax.rem(2 * turn + uu, 2 * UNROLL)

                @pl.when(dest != me)
                def _():
                    o_copy(lay, dest).start()
            return stat

        stat = lax.fori_loop(0, n_batch // UNROLL, group, jnp.zeros((32, d), F32))
        stat_t = jnp.transpose(jnp.concatenate([stat, jnp.zeros((d - 32, d), F32)], axis=0))
        st_send[:, 0, :] = jnp.where(lane32 < 32, stat_t[0:32], pltpu.roll(stat_t[64:96], 32, 1))

        each_other(lambda dest: remote(st_send.at[dest // 2], st_recv.at[lay, me], st_ssem.at[lay], st_rsem.at[lay], {'sp': dest}).start())
        mine = pl.ds(pl.multiple_of(me * 16, 16), 16)
        o_recv[lay, mine, :] = o_send[mine, :]
        st_recv[lay, me] = st_send[me // 2]
        local(kc_v.at[lay], ko_hbm.at[lay], out_sem.at[lay]).start()
        local(vc_v.at[lay], vo_hbm.at[lay], out_sem.at[2 + lay]).start()

        most = pl.ds(0, last * 16)
        remote(st_recv.at[lay, pl.ds(0, last)], st_recv.at[lay, pl.ds(0, last)], st_ssem.at[lay], st_rsem.at[lay], partner).wait_recv()
        stats = st_recv[lay, :, 0, :]
        top = jnp.max(stats, axis=0, keepdims=True)
        scale = jnp.exp(stats - top)
        denom = jnp.sum(pltpu.roll(scale, 32, 1) * stats, axis=0, keepdims=True)
        denom = pltpu.roll(jnp.broadcast_to(denom, (8, d)), d - 32, 1)
        tr_v[...] = jnp.transpose(jnp.concatenate([scale, denom, jnp.zeros((d - sp - 8, d), F32)], axis=0))
        factors = tr_v[pl.ds(pl.multiple_of(lax.rem(me, 2) * 16, 16), 16), :]
        remote(o_recv.at[lay, most], o_recv.at[lay, most], o_ssem.at[lay], o_rsem.at[lay], partner).wait_recv()
        merged = jnp.zeros((16, d), F32)
        for i in range(sp):
            merged = merged + factors[:, i:i + 1] * o_recv[lay, i * 16:i * 16 + 16, :]
        at_v[...] = merged / factors[:, sp:sp + 1]
        remote(o_send.at[most], o_send.at[most], o_ssem.at[lay], o_rsem.at[lay], partner).wait_send()
        remote(st_recv.at[lay, pl.ds(0, last)], st_recv.at[lay, pl.ds(0, last)], st_ssem.at[lay], st_rsem.at[lay], partner).wait_send()
        cols = []
        for g in range(heads):
            cols.append(jnp.concatenate([jnp.broadcast_to(at_v[g:g + 1, :], (8, d)), jnp.broadcast_to(at_v[8 + g:9 + g, :], (8, d))], axis=0))
        return jnp.concatenate(cols, axis=1).astype(BF16)

    def o_copy(lay, dest):
        return remote(o_send.at[pl.ds(pl.multiple_of(dest * 16, 16), 16)], o_recv.at[lay, pl.ds(pl.multiple_of(me * 16, 16), 16)],
                      o_ssem.at[lay], o_rsem.at[lay], {'sp': dest})

    def team_exchange(send, recv, ssem, rsem, part, slots):
        for j in range(TEAM):
            for c in range(2):
                @pl.when(jnp.logical_or(team + j != me, core != c))
                def _():
                    remote(part(j), recv.at[rank * 2 + core], ssem, rsem, {'sp': team + j, 'tp': c}).start()

        recv[rank * 2 + core] = slots
        others = remote(recv.at[pl.ds(0, 2 * TEAM - 1)], recv.at[pl.ds(0, 2 * TEAM - 1)], ssem, rsem, partner)
        others.wait_recv()
        others.wait_send()

    sub8 = iota((8, d), 0)

    def to_dense(rows):
        out = []
        for tok in range(2):
            for top in range(0, groups, 8):
                block = jnp.zeros((8, d), F32)
                for g in range(8):
                    block = jnp.where(sub8 == g, rows[tok * 8:tok * 8 + 8, (top + g) * d:(top + g + 1) * d], block)
                out.append(block)
        return jnp.concatenate(out, axis=0)

    def from_dense(dense):
        res_v[...] = dense
        cols = []
        for g in range(groups):
            cols.append(jnp.concatenate([jnp.broadcast_to(res_v[g:g + 1, :], (8, d)), jnp.broadcast_to(res_v[groups + g:groups + g + 1, :], (8, d))], axis=0))
        return jnp.concatenate(cols, axis=1)

    def finish_layer(lay, u, attn):
        local(wo_hbm.at[lay], wo_v, wo_sem.at[0]).wait()
        part = dot(attn, wo_v[...]) + jnp.where(core == 0, u, 0.0)
        if lay == 0:
            local(wo_hbm.at[1], wo_v, wo_sem.at[0]).start()
        dense = to_dense(part)
        a_send[lay] = dense
        team_exchange(a_send.at[lay], a_recv.at[lay], a_ssem.at[lay], a_rsem.at[lay], lambda j: a_send.at[lay], dense)
        gain = gm_ref[pl.ds(lay, 1), :].astype(F32)
        blocks = []
        for top in range(0, groups, 8):
            block = jnp.zeros((8, d), F32)
            for g in range(8):
                block = jnp.where(sub8 == g, gain[:, (top + g) * d:(top + g + 1) * d], block)
            blocks.append(block)
        gain = jnp.concatenate(blocks, axis=0)
        for j in range(TEAM):
            both = rounded(a_recv[lay, 2 * j] + a_recv[lay, 2 * j + 1])
            for tok in range(2):
                v = both[tok * groups:(tok + 1) * groups]
                mean = jnp.sum(jnp.sum(v * v, axis=1, keepdims=True), axis=0, keepdims=True) / width
                at = (2 * j + tok) * groups
                rows_v[at:at + groups, :] = v * lax.rsqrt(mean + EPS) * gain
        h = jnp.concatenate([rows_v[pl.ds(g, 2 * TEAM, stride=groups), :] for g in range(groups)], axis=1)
        h = jnp.concatenate([h, h], axis=0).astype(BF16)
        for copy in mlp_copies(lay):
            copy.wait()
        acts = []
        for at in range(0, share, PIECE):
            size = min(PIECE, share - at)
            gate = dot(h, wg_v[lay, :, at:at + size])
            up = dot(h, wu_v[lay, :, at:at + size])
            keep = iota((16, size), 1) >= rank * share - col - at
            acts.append(jnp.where(keep, gate * jax.nn.sigmoid(gate) * up, 0.0).astype(BF16))
        down = dot(jnp.concatenate(acts, axis=1), wd_v[lay])
        for g in range(groups):
            b_send[lay, pl.ds(g, 2 * TEAM, stride=groups), :] = down[0:8, g * d:(g + 1) * d]

        def rows_of(j):
            return pl.ds(pl.multiple_of(j * mine32, mine32), mine32)
        team_exchange(b_send.at[lay], b_recv.at[lay], b_ssem.at[lay], b_rsem.at[lay], lambda j: b_send.at[lay, rows_of(j)], b_send[lay, rows_of(rank), :])
        total = b_recv[lay, 0]
        for i in range(1, 2 * TEAM):
            total = total + b_recv[lay, i]
        mine = rounded(a_recv[lay, 2 * rank] + a_recv[lay, 2 * rank + 1])
        return rounded(mine + total)

    def wait_cache(lay):
        local(kc_hbm.at[lay], kc_v.at[lay], cache_sem.at[lay]).wait()
        local(vc_hbm.at[lay], vc_v.at[lay], cache_sem.at[2 + lay]).wait()

    wait_cache(0)
    pl.semaphore_wait(barrier, last + TEAM)

    def queries0(b):
        return q0_v[pl.ds(pl.multiple_of(b * 32, 32), 32), :]

    def rows0(b, ahead):
        return k0_v[pl.ds(ahead * n_batch + b, 1), :], v0_v[pl.ds(ahead * n_batch + b, 1), :]

    def queries1(b):
        return jnp.concatenate([qkv_recv[2 * b, 0:16, :], qkv_recv[2 * b + 1, 0:16, :]], axis=0)

    def rows1(b, ahead):
        kv = jnp.where(ahead >= 2, qkv_recv[2 * b + 1, 16:20, :], qkv_recv[2 * b, 16:20, :])
        odd = lax.rem(ahead, 2) == 1
        return jnp.where(odd, kv[1:2], kv[0:1]), jnp.where(odd, kv[3:4], kv[2:3])

    def wait_plane(step, part, ssem, rsem):
        which = lax.rem(my_plane + step, side)

        @pl.when(step == 0)
        def _():
            remote(part(plane - 1), part(plane - 1), ssem, rsem.at[which], partner).wait_recv()

        @pl.when(step != 0)
        def _():
            remote(part(plane), part(plane), ssem, rsem.at[which], partner).wait_recv()

    u = from_dense(finish_layer(0, u, attention(0, lambda step: None, queries0, rows0)))

    h = norm(u, ga_ref[pl.ds(1, 1), :].astype(F32))
    waits = qkv_copies(1)
    for copy in waits:
        copy.wait()
    sub = row16 % 8
    q = jnp.zeros((16, d), F32)
    for pair in range(heads // 2):
        both = dot(h, wqkv_v[:, pair * 256:pair * 256 + 256])
        q = jnp.where(sub == 2 * pair, both[:, :d], jnp.where(sub == 2 * pair + 1, both[:, d:], q))
    both = dot(h, wqkv_v[:, qw:qw + 256])
    qkv_send[0:16, :] = rounded(rope(q, my_cos, my_sin))
    k = rounded(rope(both[:, :d], my_cos, my_sin))
    v = rounded(both[:, d:])
    kv = jnp.where(sub8 == 0, k[:8], jnp.where(sub8 == 1, k[8:], jnp.where(sub8 == 2, v[:8], v[8:])))
    qkv_send[16:20, :] = kv[:4]
    each_other(lambda dest: remote(qkv_send, qkv_recv.at[me], ag_ssem.at[0], qkv_rsem.at[my_plane], {'sp': dest}).start())
    qkv_recv[me] = qkv_send[...]
    wait_cache(1)

    def arrive(step):
        wait_plane(step, lambda n: qkv_recv.at[pl.ds(0, n)], ag_ssem.at[0], qkv_rsem)

    u = finish_layer(1, u, attention(1, arrive, queries1, rows1))
    remote(qkv_recv.at[pl.ds(0, last)], qkv_recv.at[pl.ds(0, last)], ag_ssem.at[0], qkv_rsem.at[0], partner).wait_send()

    half = width // 2
    res_v[...] = u
    msg = jnp.concatenate([res_v[pl.ds(pl.multiple_of(tok * groups + core * 8, 8), 8), :] for tok in range(2)], axis=0)
    h_send[...] = msg

    mine = pl.ds(pl.multiple_of(me * 16, 16), 16)
    each_other(lambda dest: remote(h_send, h_recv.at[mine], ag_ssem.at[1], h_rsem.at[my_plane], {'sp': dest}).start())
    h_recv[mine, :] = h_send[...]

    def swap(step):
        rows = pl.ds(pl.multiple_of(lax.rem(my_plane + step, side) * plane * 16, plane * 16), plane * 16)
        return remote(h_recv.at[rows], h_other.at[rows], sw_ssem.at[step], sw_rsem.at[step], partner)
    for step in range(side):
        wait_plane(step, lambda n: h_recv.at[pl.ds(0, n * 16)], ag_ssem.at[1], h_rsem)
        swap(step).start()

    def spread(ref, which):
        for s in range(n_steps):
            for cg in range(8):
                rows = ref[pl.ds(s * 8 + cg, n_batch, stride=n_steps * 8), :]
                out_v[s * n_batch:(s + 1) * n_batch, pl.ds(pl.multiple_of(which * half + cg * d, d), d)] = rows.astype(BF16)
    spread(h_recv, core)
    for step in range(side):
        swap(step).wait()
    spread(h_other, 1 - core)
    done = local(out_v, hid_hbm, in_sem.at[1])
    done.start()
    most = pl.ds(0, last * 16)
    remote(h_recv.at[most], h_recv.at[most], ag_ssem.at[1], h_rsem.at[0], partner).wait_send()
    for lay in range(2):
        local(kc_v.at[lay], ko_hbm.at[lay], out_sem.at[lay]).wait()
        local(vc_v.at[lay], vo_hbm.at[lay], out_sem.at[2 + lay]).wait()
    done.wait()


def deliver_kernel(parts, *refs):
    n = len(parts)
    srcs, dsts, bufs, sems = refs[:n], refs[n:2 * n], refs[2 * n:3 * n], refs[3 * n]
    loads, stores = [], []
    for i, part in enumerate(parts):
        for j in range(srcs[i].shape[0] // part):
            rows = pl.ds(j * part, part)
            loads.append(pltpu.make_async_copy(srcs[i].at[rows], bufs[i].at[rows], sems.at[0, len(loads)]))
            stores.append(pltpu.make_async_copy(bufs[i].at[rows], dsts[i].at[rows], sems.at[1, len(stores)]))
    for load in loads:
        load.start()
    for load, store in zip(loads, stores):
        load.wait()
        store.start()
    for store in stores:
        store.wait()


def deliver(arrays):
    flat = [a.reshape(-1, a.shape[-1]) for a in arrays]
    parts = [max(a.shape[0] // 4, 16) if a.shape[0] > 1024 else a.shape[0] for a in flat]
    count = sum(a.shape[0] // part for a, part in zip(flat, parts))
    any_space = pl.BlockSpec(memory_space=pl.ANY)
    return pl.pallas_call(
        functools.partial(deliver_kernel, parts),
        out_shape=tuple(jax.ShapeDtypeStruct(a.shape, a.dtype) for a in flat),
        in_specs=[any_space] * len(flat),
        out_specs=(any_space,) * len(flat),
        scratch_shapes=[pltpu.VMEM(a.shape, a.dtype) for a in flat] + [pltpu.SemaphoreType.DMA((2, count))],
        compiler_params=pltpu.CompilerParams(vmem_limit_bytes=67043328),
        name='deliver',
    )(*flat)


def solution(mesh):
    sp = mesh.shape['sp']
    side = round(sp ** (1 / 3))

    def local_fn(tok_emb, lengths, key_cache, val_cache, gain_attn, gain_mlp, w_query, w_key, w_value, w_out, w_gate, w_up, w_down):
        n_steps, n_batch, width = tok_emb.shape
        n_layers, _, loc_len, _, d = key_cache.shape
        n_tok = n_steps * n_batch
        cache_shape = (n_layers, n_batch, loc_len, d)
        inv_freq = np.float32(1.0) / np.float32(ROPE_BASE) ** (np.arange(d // 2, dtype=np.float32) * np.float32(2.0) / np.float32(d))
        freq = jnp.asarray(np.concatenate([inv_freq, inv_freq])[None, :], F32)
        qw = w_query.shape[2]
        rows = 2 * width // d
        share = -(-w_gate.shape[2] // (d * TEAM)) * d
        vmem = pltpu.VMEM
        dma = pltpu.SemaphoreType.DMA
        in_vmem = pl.BlockSpec(memory_space=pltpu.VMEM)
        in_any = pl.BlockSpec(memory_space=pl.ANY)
        outs = pl.pallas_call(
            functools.partial(kernel, sp, n_steps, n_batch, side),
            out_shape=(jax.ShapeDtypeStruct((n_tok, width), BF16), jax.ShapeDtypeStruct(cache_shape, BF16), jax.ShapeDtypeStruct(cache_shape, BF16)),
            in_specs=[pl.BlockSpec(memory_space=pltpu.SMEM)] + [in_vmem] * 3 + [in_any] * 10,
            out_specs=(in_any,) * 3,
            scratch_shapes=[
                vmem((n_tok, width), BF16), vmem((n_tok, width), BF16), vmem((width, qw + 2 * d), BF16), vmem((qw, width), BF16),
                vmem(cache_shape, BF16), vmem(cache_shape, BF16),
                vmem((2, width, share), BF16), vmem((2, width, share), BF16), vmem((2, share, width), BF16),
                vmem((sp * 16, d), F32), vmem((n_tok, d), F32), vmem((n_tok, d), F32),
                vmem((sp, 20, d), F32),
                vmem((sp * 16, d), F32), vmem((2, sp * 16, d), F32), vmem((32, 1, d), F32), vmem((2, sp, 1, d), F32),
                vmem((2, rows, d), F32), vmem((2, 2 * TEAM, rows, d), F32), vmem((2, TEAM * rows, d), F32), vmem((2, 2 * TEAM, rows, d), F32),
                vmem((TEAM * rows, d), F32), vmem((rows, d), F32),
                vmem((20, d), F32), vmem((16, d), F32),
                vmem((sp * 16, d), F32), vmem((sp * 16, d), F32), vmem((d, d), F32), vmem((16, d), F32),
                dma((2,)), dma((4,)), dma((4,)), dma((qw // 256 + 2,)), dma((1,)), dma((2, 3)),
                dma((2,)), dma((2,)), dma((2,)), dma((2,)), dma((2,)), dma((2,)), dma((2,)), dma((2,)), dma((2,)), dma((side,)), dma((side,)), dma((side,)), dma((side,)),
            ],
            compiler_params=pltpu.CompilerParams(collective_id=0, has_side_effects=True, vmem_limit_bytes=67043328),
            name='decode',
        )(lengths, freq, gain_attn, gain_mlp, tok_emb.reshape(n_tok, width), key_cache.reshape(cache_shape), val_cache.reshape(cache_shape),
          w_query, w_key, w_value, w_out, w_gate, w_up, w_down)
        hidden, new_keys, new_vals = deliver(outs)
        return hidden.reshape(n_steps, n_batch, width), new_keys.reshape(key_cache.shape), new_vals.reshape(val_cache.shape)

    cache_spec = P(None, 'dp', 'sp', 'tp', None)
    col_spec = P(None, None, 'tp')
    row_spec = P(None, 'tp', None)
    emb_spec = P(None, 'dp', None)
    return jax.shard_map(local_fn, mesh=mesh, in_specs=(emb_spec, P('dp'), cache_spec, cache_spec, P(), P(), col_spec, col_spec, col_spec, row_spec, col_spec, col_spec, row_spec), out_specs=(emb_spec, cache_spec, cache_spec), check_vma=False)
```

```python
import functools

import jax
import jax.numpy as jnp
import numpy as np
from jax import lax
from jax.experimental import pallas as pl
from jax.experimental.pallas import tpu as pltpu
from jax.sharding import PartitionSpec as P

EPS = 1e-5
ROPE_BASE = 500000.0
TEAM = 4
PIECE = 512
UNROLL = 8
F32 = jnp.float32
BF16 = jnp.bfloat16
MESH = pl.DeviceIdType.MESH


def dot(a, b):
    return jnp.dot(a, b, preferred_element_type=F32)


def norm(u, gain):
    inv = lax.rsqrt(jnp.mean(u * u, axis=-1, keepdims=True) + EPS)
    return (u * inv * gain).astype(BF16)


def iota(shape, dim):
    return lax.broadcasted_iota(jnp.int32, shape, dim)


def kernel(sp, n_steps, n_batch, side,
           len_ref, freq_ref, ga_ref, gm_ref, x_hbm, kc_hbm, vc_hbm, wq_hbm, wk_hbm, wv_hbm, wo_hbm, wg_hbm, wu_hbm, wd_hbm,
           hid_hbm, ko_hbm, vo_hbm,
           x_v, xn_v, wqkv_v, wo_v, kc_v, vc_v, wg_v, wu_v, wd_v, q0_v, k0_v, v0_v,
           qkv_recv, o_send, o_recv, st_send, st_recv, a_send, a_recv, b_send, b_recv, rows_v, res_v, qkv_send, h_send,
           h_recv, h_other, tr_v, at_v,
           in_sem, cache_sem, out_sem, wqkv_sem, wo_sem, mlp_sem,
           o_ssem, o_rsem, st_ssem, st_rsem, a_ssem, a_rsem, b_ssem, b_rsem, ag_ssem, qkv_rsem, h_rsem, sw_ssem, sw_rsem):
    me = lax.axis_index('sp')
    core = lax.axis_index('tp')
    n_tok = n_steps * n_batch
    width = x_v.shape[1]
    d = 128
    ff = wg_hbm.shape[2]
    heads = wq_hbm.shape[2] // d
    qw = heads * d
    share = wg_v.shape[2]
    team = me // TEAM * TEAM
    rank = lax.rem(me, TEAM)
    col = pl.multiple_of(jnp.minimum(rank * share, ff - share), d)
    groups = width // d
    mine32 = 2 * groups
    last = sp - 1
    partner = {'tp': 1 - core}
    plane = side * side
    my_plane = me // plane
    out_v = x_v

    def local(src, dst, sem):
        return pltpu.make_async_copy(src, dst, sem)

    def remote(src, dst, ssem, rsem, dev):
        return pltpu.make_async_remote_copy(src_ref=src, dst_ref=dst, send_sem=ssem, recv_sem=rsem, device_id=dev, device_id_type=MESH)

    def qkv_copies(lay):
        copies = [local(wq_hbm.at[lay, :, pl.ds(i * 256, 256)], wqkv_v.at[:, pl.ds(i * 256, 256)], wqkv_sem.at[i]) for i in range(qw // 256)]
        copies.append(local(wk_hbm.at[lay], wqkv_v.at[:, pl.ds(qw, d)], wqkv_sem.at[qw // 256]))
        copies.append(local(wv_hbm.at[lay], wqkv_v.at[:, pl.ds(qw + d, d)], wqkv_sem.at[qw // 256 + 1]))
        return copies

    def each_other(send):
        many = 9 if last % 9 == 0 else 1

        def body(i, carry):
            for j in range(many):
                send(lax.rem(me + 1 + lax.rem(i * many + j + sp // 2 - 1, last), sp))
            return carry
        lax.fori_loop(0, last // many, body, 0)

    def mlp_copies(lay):
        return (local(wg_hbm.at[lay, :, pl.ds(col, share)], wg_v.at[lay], mlp_sem.at[lay, 0]),
                local(wu_hbm.at[lay, :, pl.ds(col, share)], wu_v.at[lay], mlp_sem.at[lay, 1]),
                local(wd_hbm.at[lay, pl.ds(col, share), :], wd_v.at[lay], mlp_sem.at[lay, 2]))

    def start_cache(lay):
        local(kc_hbm.at[lay], kc_v.at[lay], cache_sem.at[lay]).start()
        local(vc_hbm.at[lay], vc_v.at[lay], cache_sem.at[2 + lay]).start()

    x_copy = local(x_hbm, x_v, in_sem.at[0])
    x_copy.start()
    for copy in qkv_copies(0):
        copy.start()
    start_cache(0)
    barrier = pltpu.get_barrier_semaphore()
    each_other(lambda dest: pl.semaphore_signal(barrier, inc=1, device_id={'sp': dest}, device_id_type=MESH))
    for j in range(TEAM):
        pl.semaphore_signal(barrier, inc=1, device_id={'sp': team + j, 'tp': 1 - core}, device_id_type=MESH)

    lane = iota((1, d), 1)
    sign = jnp.where(lane < d // 2, -1.0, 1.0).astype(F32)
    freq = freq_ref[...]
    brow = iota((n_batch, d), 0)

    def place(b, acc):
        return jnp.where(brow == b, len_ref[b], acc)
    pos_b = lax.fori_loop(0, n_batch, place, jnp.zeros((n_batch, d), jnp.int32))
    angles = jnp.concatenate([(pos_b + s).astype(F32) * freq for s in range(n_steps)], axis=0)
    cos_t = jnp.cos(angles)
    sin_t = jnp.sin(angles) * sign
    row16 = iota((16, d), 0)
    my_pos = len_ref[me // 2] + 2 * lax.rem(me, 2) + row16 // 8
    my_angles = my_pos.astype(F32) * freq
    my_cos = jnp.cos(my_angles)
    my_sin = jnp.sin(my_angles) * sign

    def rope(v, c, s):
        return v * c + pltpu.roll(v, d // 2, 1) * s

    def rounded(v):
        return v.astype(BF16).astype(F32)

    x_copy.wait()
    xn_v[...] = norm(x_v[...].astype(F32), ga_ref[pl.ds(0, 1), :].astype(F32))
    xn = xn_v[...]
    waits = qkv_copies(0)
    for pair in range(heads // 2):
        waits[pair].wait()
        both = dot(xn, wqkv_v[:, pair * 256:pair * 256 + 256])
        for g in (2 * pair, 2 * pair + 1):
            off = (g % 2) * d
            q = rounded(rope(both[:, off:off + d], cos_t, sin_t))
            for s in range(n_steps):
                q0_v[pl.ds(s * heads + g, n_batch, stride=n_steps * heads), :] = q[s * n_batch:(s + 1) * n_batch]
    waits[-2].wait()
    waits[-1].wait()
    both = dot(xn, wqkv_v[:, qw:qw + 256])
    k0_v[...] = rounded(rope(both[:, :d], cos_t, sin_t))
    v0_v[...] = rounded(both[:, d:])
    own_row = (2 * lax.rem(me, 2) + iota((16, n_tok), 0) // 8) * n_batch + me // 2
    pick = jnp.where(iota((16, n_tok), 1) == own_row, 1.0, 0.0).astype(BF16)
    u = dot(pick, x_v[...])

    pos_row = iota((32, d), 1) * sp + me - iota((32, d), 0) // heads
    lane32 = iota((32, d), 1)
    slot_rows = iota((d, d), 0).astype(F32).astype(BF16)

    def attention(lay, arrive, queries, new_rows):
        def group(step, stat):
            first = lax.rem(my_plane + step, side) * UNROLL
            turn = lax.rem(me, plane) // 2
            arrive(step)
            for uu in range(UNROLL):
                b = first + lax.rem(turn + uu, UNROLL)
                length = len_ref[b]
                ahead = lax.rem(me - length + 1024 * sp, sp)
                slot = jnp.where(ahead < n_steps, (length + ahead) // sp, -1)
                hit = slot_rows == jnp.full((d, d), slot.astype(F32)).astype(BF16)
                k_row, v_row = new_rows(b, jnp.minimum(ahead, n_steps - 1))
                k_new = jnp.where(hit, jnp.broadcast_to(k_row, (d, d)).astype(BF16), kc_v[lay, b])
                v_new = jnp.where(hit, jnp.broadcast_to(v_row, (d, d)).astype(BF16), vc_v[lay, b])
                kc_v[lay, b] = k_new
                vc_v[lay, b] = v_new
                rows = pl.ds(pl.multiple_of(b * 32, 32), 32)
                q = queries(b).astype(BF16)
                s = lax.dot_general(q, k_new, (((1,), (1,)), ((), ())), preferred_element_type=F32) * (d ** -0.5)
                s = jnp.where(pos_row <= length, s, -1e30)
                m = jnp.max(s, axis=-1, keepdims=True)
                w = jnp.exp(s - m)
                l = jnp.sum(w, axis=-1, keepdims=True)
                o_send[rows, :] = dot(w.astype(BF16), v_new)
                stat = jnp.where(lane32 == b, m, jnp.where(lane32 == 64 + b, l, stat))
            for uu in range(2 * UNROLL):
                dest = 2 * first + lax.rem(2 * turn + uu, 2 * UNROLL)

                @pl.when(dest != me)
                def _():
                    o_copy(lay, dest).start()
            return stat

        stat = lax.fori_loop(0, n_batch // UNROLL, group, jnp.zeros((32, d), F32))
        stat_t = jnp.transpose(jnp.concatenate([stat, jnp.zeros((d - 32, d), F32)], axis=0))
        st_send[:, 0, :] = jnp.where(lane32 < 32, stat_t[0:32], pltpu.roll(stat_t[64:96], 32, 1))

        each_other(lambda dest: remote(st_send.at[dest // 2], st_recv.at[lay, me], st_ssem.at[lay], st_rsem.at[lay], {'sp': dest}).start())
        mine = pl.ds(pl.multiple_of(me * 16, 16), 16)
        o_recv[lay, mine, :] = o_send[mine, :]
        st_recv[lay, me] = st_send[me // 2]
        local(kc_v.at[lay], ko_hbm.at[lay], out_sem.at[lay]).start()
        local(vc_v.at[lay], vo_hbm.at[lay], out_sem.at[2 + lay]).start()

        most = pl.ds(0, last * 16)
        remote(st_recv.at[lay, pl.ds(0, last)], st_recv.at[lay, pl.ds(0, last)], st_ssem.at[lay], st_rsem.at[lay], partner).wait_recv()
        stats = st_recv[lay, :, 0, :]
        top = jnp.max(stats, axis=0, keepdims=True)
        scale = jnp.exp(stats - top)
        denom = jnp.sum(pltpu.roll(scale, 32, 1) * stats, axis=0, keepdims=True)
        denom = pltpu.roll(jnp.broadcast_to(denom, (8, d)), d - 32, 1)
        tr_v[...] = jnp.transpose(jnp.concatenate([scale, denom, jnp.zeros((d - sp - 8, d), F32)], axis=0))
        factors = tr_v[pl.ds(pl.multiple_of(lax.rem(me, 2) * 16, 16), 16), :]
        remote(o_recv.at[lay, most], o_recv.at[lay, most], o_ssem.at[lay], o_rsem.at[lay], partner).wait_recv()
        merged = jnp.zeros((16, d), F32)
        for i in range(sp):
            merged = merged + factors[:, i:i + 1] * o_recv[lay, i * 16:i * 16 + 16, :]
        at_v[...] = merged / factors[:, sp:sp + 1]
        remote(o_send.at[most], o_send.at[most], o_ssem.at[lay], o_rsem.at[lay], partner).wait_send()
        remote(st_recv.at[lay, pl.ds(0, last)], st_recv.at[lay, pl.ds(0, last)], st_ssem.at[lay], st_rsem.at[lay], partner).wait_send()
        cols = []
        for g in range(heads):
            cols.append(jnp.concatenate([jnp.broadcast_to(at_v[g:g + 1, :], (8, d)), jnp.broadcast_to(at_v[8 + g:9 + g, :], (8, d))], axis=0))
        return jnp.concatenate(cols, axis=1).astype(BF16)

    def o_copy(lay, dest):
        return remote(o_send.at[pl.ds(pl.multiple_of(dest * 16, 16), 16)], o_recv.at[lay, pl.ds(pl.multiple_of(me * 16, 16), 16)],
                      o_ssem.at[lay], o_rsem.at[lay], {'sp': dest})

    def team_exchange(send, recv, ssem, rsem, part, slots):
        for j in range(TEAM):
            for c in range(2):
                @pl.when(jnp.logical_or(team + j != me, core != c))
                def _():
                    remote(part(j), recv.at[rank * 2 + core], ssem, rsem, {'sp': team + j, 'tp': c}).start()

        recv[rank * 2 + core] = slots
        others = remote(recv.at[pl.ds(0, 2 * TEAM - 1)], recv.at[pl.ds(0, 2 * TEAM - 1)], ssem, rsem, partner)
        others.wait_recv()
        others.wait_send()

    sub8 = iota((8, d), 0)

    def to_dense(rows):
        out = []
        for tok in range(2):
            for top in range(0, groups, 8):
                block = jnp.zeros((8, d), F32)
                for g in range(8):
                    block = jnp.where(sub8 == g, rows[tok * 8:tok * 8 + 8, (top + g) * d:(top + g + 1) * d], block)
                out.append(block)
        return jnp.concatenate(out, axis=0)

    def from_dense(dense):
        res_v[...] = dense
        cols = []
        for g in range(groups):
            cols.append(jnp.concatenate([jnp.broadcast_to(res_v[g:g + 1, :], (8, d)), jnp.broadcast_to(res_v[groups + g:groups + g + 1, :], (8, d))], axis=0))
        return jnp.concatenate(cols, axis=1)

    def finish_layer(lay, u, attn):
        local(wo_hbm.at[lay], wo_v, wo_sem.at[0]).wait()
        part = dot(attn, wo_v[...]) + jnp.where(core == 0, u, 0.0)
        if lay == 0:
            local(wo_hbm.at[1], wo_v, wo_sem.at[0]).start()
        dense = to_dense(part)
        a_send[lay] = dense
        team_exchange(a_send.at[lay], a_recv.at[lay], a_ssem.at[lay], a_rsem.at[lay], lambda j: a_send.at[lay], dense)
        gain = gm_ref[pl.ds(lay, 1), :].astype(F32)
        blocks = []
        for top in range(0, groups, 8):
            block = jnp.zeros((8, d), F32)
            for g in range(8):
                block = jnp.where(sub8 == g, gain[:, (top + g) * d:(top + g + 1) * d], block)
            blocks.append(block)
        gain = jnp.concatenate(blocks, axis=0)
        for j in range(TEAM):
            both = rounded(a_recv[lay, 2 * j] + a_recv[lay, 2 * j + 1])
            for tok in range(2):
                v = both[tok * groups:(tok + 1) * groups]
                mean = jnp.sum(jnp.sum(v * v, axis=1, keepdims=True), axis=0, keepdims=True) / width
                at = (2 * j + tok) * groups
                rows_v[at:at + groups, :] = v * lax.rsqrt(mean + EPS) * gain
        h = jnp.concatenate([rows_v[pl.ds(g, 2 * TEAM, stride=groups), :] for g in range(groups)], axis=1)
        h = jnp.concatenate([h, h], axis=0).astype(BF16)
        for copy in mlp_copies(lay):
            copy.wait()
        if lay == 0:
            for copy in mlp_copies(1):
                copy.start()
        acts = []
        for at in range(0, share, PIECE):
            size = min(PIECE, share - at)
            gate = dot(h, wg_v[lay, :, at:at + size])
            up = dot(h, wu_v[lay, :, at:at + size])
            keep = iota((16, size), 1) >= rank * share - col - at
            acts.append(jnp.where(keep, gate * jax.nn.sigmoid(gate) * up, 0.0).astype(BF16))
        down = dot(jnp.concatenate(acts, axis=1), wd_v[lay])
        for g in range(groups):
            b_send[lay, pl.ds(g, 2 * TEAM, stride=groups), :] = down[0:8, g * d:(g + 1) * d]

        def rows_of(j):
            return pl.ds(pl.multiple_of(j * mine32, mine32), mine32)
        team_exchange(b_send.at[lay], b_recv.at[lay], b_ssem.at[lay], b_rsem.at[lay], lambda j: b_send.at[lay, rows_of(j)], b_send[lay, rows_of(rank), :])
        total = b_recv[lay, 0]
        for i in range(1, 2 * TEAM):
            total = total + b_recv[lay, i]
        mine = rounded(a_recv[lay, 2 * rank] + a_recv[lay, 2 * rank + 1])
        return rounded(mine + total)

    def wait_cache(lay):
        local(kc_hbm.at[lay], kc_v.at[lay], cache_sem.at[lay]).wait()
        local(vc_hbm.at[lay], vc_v.at[lay], cache_sem.at[2 + lay]).wait()

    wait_cache(0)

    local(wo_hbm.at[0], wo_v, wo_sem.at[0]).start()
    for copy in mlp_copies(0):
        copy.start()
    for copy in qkv_copies(1):
        copy.start()
    start_cache(1)
    pl.semaphore_wait(barrier, last + TEAM)

    def queries0(b):
        return q0_v[pl.ds(pl.multiple_of(b * 32, 32), 32), :]

    def rows0(b, ahead):
        return k0_v[pl.ds(ahead * n_batch + b, 1), :], v0_v[pl.ds(ahead * n_batch + b, 1), :]

    def queries1(b):
        return jnp.concatenate([qkv_recv[2 * b, 0:16, :], qkv_recv[2 * b + 1, 0:16, :]], axis=0)

    def rows1(b, ahead):
        kv = jnp.where(ahead >= 2, qkv_recv[2 * b + 1, 16:20, :], qkv_recv[2 * b, 16:20, :])
        odd = lax.rem(ahead, 2) == 1
        return jnp.where(odd, kv[1:2], kv[0:1]), jnp.where(odd, kv[3:4], kv[2:3])

    def wait_plane(step, part, ssem, rsem):
        which = lax.rem(my_plane + step, side)

        @pl.when(step == 0)
        def _():
            remote(part(plane - 1), part(plane - 1), ssem, rsem.at[which], partner).wait_recv()

        @pl.when(step != 0)
        def _():
            remote(part(plane), part(plane), ssem, rsem.at[which], partner).wait_recv()

    u = from_dense(finish_layer(0, u, attention(0, lambda step: None, queries0, rows0)))

    h = norm(u, ga_ref[pl.ds(1, 1), :].astype(F32))
    waits = qkv_copies(1)
    for copy in waits:
        copy.wait()
    sub = row16 % 8
    q = jnp.zeros((16, d), F32)
    for pair in range(heads // 2):
        both = dot(h, wqkv_v[:, pair * 256:pair * 256 + 256])
        q = jnp.where(sub == 2 * pair, both[:, :d], jnp.where(sub == 2 * pair + 1, both[:, d:], q))
    both = dot(h, wqkv_v[:, qw:qw + 256])
    qkv_send[0:16, :] = rounded(rope(q, my_cos, my_sin))
    k = rounded(rope(both[:, :d], my_cos, my_sin))
    v = rounded(both[:, d:])
    kv = jnp.where(sub8 == 0, k[:8], jnp.where(sub8 == 1, k[8:], jnp.where(sub8 == 2, v[:8], v[8:])))
    qkv_send[16:20, :] = kv[:4]
    each_other(lambda dest: remote(qkv_send, qkv_recv.at[me], ag_ssem.at[0], qkv_rsem.at[my_plane], {'sp': dest}).start())
    qkv_recv[me] = qkv_send[...]
    wait_cache(1)

    def arrive(step):
        wait_plane(step, lambda n: qkv_recv.at[pl.ds(0, n)], ag_ssem.at[0], qkv_rsem)

    u = finish_layer(1, u, attention(1, arrive, queries1, rows1))
    remote(qkv_recv.at[pl.ds(0, last)], qkv_recv.at[pl.ds(0, last)], ag_ssem.at[0], qkv_rsem.at[0], partner).wait_send()

    half = width // 2
    res_v[...] = u
    msg = jnp.concatenate([res_v[pl.ds(pl.multiple_of(tok * groups + core * 8, 8), 8), :] for tok in range(2)], axis=0)
    h_send[...] = msg

    mine = pl.ds(pl.multiple_of(me * 16, 16), 16)
    each_other(lambda dest: remote(h_send, h_recv.at[mine], ag_ssem.at[1], h_rsem.at[my_plane], {'sp': dest}).start())
    h_recv[mine, :] = h_send[...]

    def swap(step):
        rows = pl.ds(pl.multiple_of(lax.rem(my_plane + step, side) * plane * 16, plane * 16), plane * 16)
        return remote(h_recv.at[rows], h_other.at[rows], sw_ssem.at[step], sw_rsem.at[step], partner)
    for step in range(side):
        wait_plane(step, lambda n: h_recv.at[pl.ds(0, n * 16)], ag_ssem.at[1], h_rsem)
        swap(step).start()

    def spread(ref, which):
        for s in range(n_steps):
            for cg in range(8):
                rows = ref[pl.ds(s * 8 + cg, n_batch, stride=n_steps * 8), :]
                out_v[s * n_batch:(s + 1) * n_batch, pl.ds(pl.multiple_of(which * half + cg * d, d), d)] = rows.astype(BF16)
    spread(h_recv, core)
    for step in range(side):
        swap(step).wait()
    spread(h_other, 1 - core)
    done = local(out_v, hid_hbm, in_sem.at[1])
    done.start()
    most = pl.ds(0, last * 16)
    remote(h_recv.at[most], h_recv.at[most], ag_ssem.at[1], h_rsem.at[0], partner).wait_send()
    for lay in range(2):
        local(kc_v.at[lay], ko_hbm.at[lay], out_sem.at[lay]).wait()
        local(vc_v.at[lay], vo_hbm.at[lay], out_sem.at[2 + lay]).wait()
    done.wait()


def deliver_kernel(parts, *refs):
    n = len(parts)
    srcs, dsts, bufs, sems = refs[:n], refs[n:2 * n], refs[2 * n:3 * n], refs[3 * n]
    loads, stores = [], []
    for i, part in enumerate(parts):
        for j in range(srcs[i].shape[0] // part):
            rows = pl.ds(j * part, part)
            loads.append(pltpu.make_async_copy(srcs[i].at[rows], bufs[i].at[rows], sems.at[0, len(loads)]))
            stores.append(pltpu.make_async_copy(bufs[i].at[rows], dsts[i].at[rows], sems.at[1, len(stores)]))
    for load in loads:
        load.start()
    for load, store in zip(loads, stores):
        load.wait()
        store.start()
    for store in stores:
        store.wait()


def deliver(arrays):
    flat = [a.reshape(-1, a.shape[-1]) for a in arrays]
    parts = [max(a.shape[0] // 4, 16) if a.shape[0] > 1024 else a.shape[0] for a in flat]
    count = sum(a.shape[0] // part for a, part in zip(flat, parts))
    any_space = pl.BlockSpec(memory_space=pl.ANY)
    return pl.pallas_call(
        functools.partial(deliver_kernel, parts),
        out_shape=tuple(jax.ShapeDtypeStruct(a.shape, a.dtype) for a in flat),
        in_specs=[any_space] * len(flat),
        out_specs=(any_space,) * len(flat),
        scratch_shapes=[pltpu.VMEM(a.shape, a.dtype) for a in flat] + [pltpu.SemaphoreType.DMA((2, count))],
        compiler_params=pltpu.CompilerParams(vmem_limit_bytes=67043328),
        name='deliver',
    )(*flat)


def solution(mesh):
    sp = mesh.shape['sp']
    side = round(sp ** (1 / 3))

    def local_fn(tok_emb, lengths, key_cache, val_cache, gain_attn, gain_mlp, w_query, w_key, w_value, w_out, w_gate, w_up, w_down):
        n_steps, n_batch, width = tok_emb.shape
        n_layers, _, loc_len, _, d = key_cache.shape
        n_tok = n_steps * n_batch
        cache_shape = (n_layers, n_batch, loc_len, d)
        inv_freq = np.float32(1.0) / np.float32(ROPE_BASE) ** (np.arange(d // 2, dtype=np.float32) * np.float32(2.0) / np.float32(d))
        freq = jnp.asarray(np.concatenate([inv_freq, inv_freq])[None, :], F32)
        qw = w_query.shape[2]
        rows = 2 * width // d
        share = -(-w_gate.shape[2] // (d * TEAM)) * d
        vmem = pltpu.VMEM
        dma = pltpu.SemaphoreType.DMA
        in_vmem = pl.BlockSpec(memory_space=pltpu.VMEM)
        in_any = pl.BlockSpec(memory_space=pl.ANY)
        outs = pl.pallas_call(
            functools.partial(kernel, sp, n_steps, n_batch, side),
            out_shape=(jax.ShapeDtypeStruct((n_tok, width), BF16), jax.ShapeDtypeStruct(cache_shape, BF16), jax.ShapeDtypeStruct(cache_shape, BF16)),
            in_specs=[pl.BlockSpec(memory_space=pltpu.SMEM)] + [in_vmem] * 3 + [in_any] * 10,
            out_specs=(in_any,) * 3,
            scratch_shapes=[
                vmem((n_tok, width), BF16), vmem((n_tok, width), BF16), vmem((width, qw + 2 * d), BF16), vmem((qw, width), BF16),
                vmem(cache_shape, BF16), vmem(cache_shape, BF16),
                vmem((2, width, share), BF16), vmem((2, width, share), BF16), vmem((2, share, width), BF16),
                vmem((sp * 16, d), F32), vmem((n_tok, d), F32), vmem((n_tok, d), F32),
                vmem((sp, 20, d), F32),
                vmem((sp * 16, d), F32), vmem((2, sp * 16, d), F32), vmem((32, 1, d), F32), vmem((2, sp, 1, d), F32),
                vmem((2, rows, d), F32), vmem((2, 2 * TEAM, rows, d), F32), vmem((2, TEAM * rows, d), F32), vmem((2, 2 * TEAM, rows, d), F32),
                vmem((TEAM * rows, d), F32), vmem((rows, d), F32),
                vmem((20, d), F32), vmem((16, d), F32),
                vmem((sp * 16, d), F32), vmem((sp * 16, d), F32), vmem((d, d), F32), vmem((16, d), F32),
                dma((2,)), dma((4,)), dma((4,)), dma((qw // 256 + 2,)), dma((1,)), dma((2, 3)),
                dma((2,)), dma((2,)), dma((2,)), dma((2,)), dma((2,)), dma((2,)), dma((2,)), dma((2,)), dma((2,)), dma((side,)), dma((side,)), dma((side,)), dma((side,)),
            ],
            compiler_params=pltpu.CompilerParams(collective_id=0, has_side_effects=True, vmem_limit_bytes=67043328),
            name='decode',
        )(lengths, freq, gain_attn, gain_mlp, tok_emb.reshape(n_tok, width), key_cache.reshape(cache_shape), val_cache.reshape(cache_shape),
          w_query, w_key, w_value, w_out, w_gate, w_up, w_down)
        hidden, new_keys, new_vals = deliver(outs)
        return hidden.reshape(n_steps, n_batch, width), new_keys.reshape(key_cache.shape), new_vals.reshape(val_cache.shape)

    cache_spec = P(None, 'dp', 'sp', 'tp', None)
    col_spec = P(None, None, 'tp')
    row_spec = P(None, 'tp', None)
    emb_spec = P(None, 'dp', None)
    return jax.shard_map(local_fn, mesh=mesh, in_specs=(emb_spec, P('dp'), cache_spec, cache_spec, P(), P(), col_spec, col_spec, col_spec, row_spec, col_spec, col_spec, row_spec), out_specs=(emb_spec, cache_spec, cache_spec), check_vma=False)
```
